32 devices in a mesh: row: 8 (over z, x), col: 4 (over y, core).
Axes of the slice: x: 2, y: 2, z: 4, core: 2. Of those that a mesh axis runs over, the one named last changes fastest.
Arguments:
- front_pivot: float32 [64, 128, 128], P('col', 'row'), may hold values from -256 to 256, as said below
- front_update: float32 [64, 640, 768], P('col', 'row'), may hold values from -12 to 12, as said below
- child_blocks: float32 [64, 2, 512, 512], P('col', None, 'row'), may hold values from -0.5 to 0.5, as said below
- child_map: int32 [64, 2, 512], P('col'), may hold values from -1 to 767, as said below
Outputs:
- lhat: float32 [64, 640, 128], P('col', 'row')
- schur: float32 [64, 640, 640], P('col', 'row')
- negative_share: float32 [], replicated
The draws below stay inside these ranges and needn't reach their ends.
Inputs may be any that keep to these rules, and one draw needn't show every extreme that they name: `front_pivot`: symmetric in its last two dimensions. With both children's entries added, the pivot block of every front has an LDL^T factorization without pivoting whose pivots have magnitudes 4 to 40. `front_update`: the last 640 columns of each front form a symmetric matrix. `child_blocks`: symmetric in its last two dimensions. child_map[f, c, i] is the row and column of front f's assembled matrix that row and column i of child c go to, or -1 for padding. A child's entries of 0 or more are distinct, come before its padding, and number at least 385, and more than half of 512. Parent row p is held by grid row p // 16 if p < 128, else by (p - 128) // 80. Of the 64 rows i of a child with the same i // 64, at most 16 go to rows held by any one grid row, and every child reaches that bound.
All inputs are finite; a program needn't handle non-finite values.
Results may differ from the reference program's by a relative error of at most 0.0003.
Values sent between devices are 32-bit elements; how exact they have to be, the bound alone decides.
No kernel may reach another device: no remote copies, remote signals or barrier semaphores. Data moves between devices by JAX's collectives and lax.ppermute only.
A program may use at most 64 MiB of HBM per device.

```python
import jax
import jax.numpy as jnp
from jax import lax

F = 768
S = 128
CU = 512
U = 640
NFRONT = 64
SP = 16
UP = 80
HELD = 64
CAP = 16
N_ROW = 8


def draw_front_pivot(key, part):
    key_list = jax.random.split(jax.random.fold_in(key, 11), 3)
    reach = 1.2 * (3.0 / S) ** 0.5
    entries = jax.random.uniform(key_list[0], (NFRONT, S, S), jnp.float32, -reach, reach)
    index = jnp.arange(S, dtype=jnp.int32)
    strict = index[:, None] > index[None, :]
    unit_factor = jnp.where(strict[None, :, :], entries, jnp.zeros_like(entries)) + jnp.eye(S, dtype=jnp.float32)[None, :, :]
    logs = jax.random.uniform(key_list[1], (NFRONT, S), jnp.float32, jnp.log(4.0), jnp.log(40.0))
    magnitude = jnp.exp(logs)
    neg_rate = 0.15 + 0.45 * jnp.arange(NFRONT, dtype=jnp.float32) / max(NFRONT - 1, 1)
    negative = jax.random.uniform(key_list[2], (NFRONT, S), jnp.float32) < neg_rate[:, None]
    pivots = jnp.where(negative, -magnitude, magnitude)
    target = jnp.einsum('fik,fjk->fij', unit_factor * pivots[:, None, :], unit_factor, precision=lax.Precision.HIGHEST)
    target = 0.5 * (target + jnp.swapaxes(target, 1, 2))
    blocks = draw_child_blocks(key, part)
    maps = draw_child_map(key, part)
    slots = jnp.arange(S, dtype=jnp.int32)
    hot = (maps[:, :, None, :] == slots[None, None, :, None]).astype(jnp.float32)
    spread = jnp.einsum('fcpi,fcij->fcpj', hot, blocks, precision=lax.Precision.HIGHEST)
    added = jnp.einsum('fcpj,fcqj->fpq', spread, hot, precision=lax.Precision.HIGHEST)
    return (target - added).astype(jnp.float32)


def draw_front_update(key, part):
    key_list = jax.random.split(jax.random.fold_in(key, 23), 1)
    values = jnp.clip(2.0 * jax.random.normal(key_list[0], (NFRONT, U, F), jnp.float32), -8.0, 8.0)
    coupling = values[:, :, :S]
    trailing = values[:, :, S:]
    trailing = (trailing + jnp.swapaxes(trailing, 1, 2)) * 0.7071
    return jnp.concatenate([coupling, trailing], axis=2).astype(jnp.float32)


def draw_child_blocks(key, part):
    key_list = jax.random.split(jax.random.fold_in(key, 31), 1)
    random_part = jax.random.uniform(key_list[0], (NFRONT, 2, CU, CU), jnp.float32, -0.5, 0.5)
    return (0.5 * (random_part + jnp.swapaxes(random_part, 2, 3))).astype(jnp.float32)


def draw_child_map(key, part):
    lowest = max(CU - 127, CU // 2 + 1)

    def one_child(child_key):
        key_list = jax.random.split(child_key, 3)
        count = jax.random.randint(key_list[0], (), lowest, CU + 1)
        offsets = jax.random.permutation(key_list[1], N_ROW)[:N_ROW // 2]
        targets = jax.vmap(lambda inner: jax.random.permutation(inner, SP + UP)[:HELD])(jax.random.split(key_list[2], N_ROW))
        position = jnp.arange(CU, dtype=jnp.int32)
        source = position // HELD
        within = position % HELD
        group = within // CAP
        owner = (source + offsets[group]) % N_ROW
        local = targets[owner, within]
        parent = jnp.where(local < SP, owner * SP + local, S + owner * UP + local - SP)
        return jnp.where(position < count, parent, -1).astype(jnp.int32)
    key_list = jax.random.split(jax.random.fold_in(key, 37), NFRONT * 2)
    return jax.vmap(one_child)(key_list).reshape(NFRONT, 2, CU).astype(jnp.int32)


def setup_inputs(seed: int = 0) -> dict:
    keys = jax.random.split(jax.random.key(seed), 5)
    front_pivot = draw_front_pivot(jax.random.fold_in(keys[4], 71), 0)
    front_update = draw_front_update(jax.random.fold_in(keys[4], 71), 0)
    child_blocks = draw_child_blocks(jax.random.fold_in(keys[4], 71), 0)
    child_map = draw_child_map(jax.random.fold_in(keys[4], 71), 0)
    return {"front_pivot": front_pivot, "front_update": front_update, "child_blocks": child_blocks, "child_map": child_map}


highest = lax.Precision.HIGHEST

def factor(blocks):
    count = blocks.shape[-1]
    index = jnp.arange(count, dtype=jnp.int32)

    def eliminate(column_index, carry):
        current, pivots = carry
        column = lax.dynamic_index_in_dim(current, column_index, 2, keepdims=False)
        leading = lax.dynamic_index_in_dim(current, column_index, 1, keepdims=False)
        pivot = lax.dynamic_index_in_dim(column, column_index, 1, keepdims=False)
        below = index[None, :] > column_index
        multiplier = jnp.where(below, column / pivot[:, None], jnp.zeros_like(column))
        current = current - multiplier[:, :, None] * leading[:, None, :]
        pivots = jnp.where(index[None, :] == column_index, pivot[:, None], pivots)
        return (current, pivots)
    start = (blocks, jnp.zeros(blocks.shape[:2], blocks.dtype))
    current, pivots = lax.fori_loop(0, count, eliminate, start)
    upper = jnp.where(index[:, None] <= index[None, :], current, jnp.zeros_like(current)) / pivots[:, :, None]
    lower = jnp.swapaxes(upper, 1, 2)
    identity = jnp.eye(count, dtype=blocks.dtype)
    inverse = jax.vmap(lambda matrix: jax.scipy.linalg.solve_triangular(matrix, identity, lower=True, unit_diagonal=True))(lower)
    return (inverse, pivots)

def assemble(inputs):
    pivot_rows, update_rows, blocks, indices = inputs
    upper_rows = jnp.concatenate([pivot_rows, jnp.swapaxes(update_rows[:, :S], 0, 1)], axis=1)
    whole = jnp.concatenate([upper_rows, update_rows], axis=0)
    for child in range(2):
        spot = jnp.where(indices[child] >= 0, indices[child], F).astype(jnp.int32)
        whole = whole.at[spot[:, None], spot[None, :]].add(blocks[child], mode='drop')
    return (whole[:S, :S], whole[S:, :S], whole[S:, S:])

def reference(front_pivot, front_update, child_blocks, child_map):
    pivot_block, coupling, trailing = lax.map(assemble, (front_pivot, front_update, child_blocks, child_map))
    inverse, pivots = factor(pivot_block)
    lhat = jnp.einsum('fik,fjk->fij', coupling, inverse, precision=highest)
    scaled = lhat / pivots[:, None, :]
    schur = trailing - jnp.einsum('fik,fjk->fij', scaled, lhat, precision=highest)
    negatives = jnp.sum(jnp.where(pivots < 0.0, 1.0, 0.0).astype(jnp.float32))
    negative_share = (negatives / (NFRONT * S)).astype(jnp.float32)
    return (lhat, schur, negative_share)
```

```python
import functools

import jax
import jax.numpy as jnp
from jax import lax
from jax.experimental import pallas as pl
from jax.experimental.pallas import tpu as pltpu
from jax.sharding import PartitionSpec as P

LANES = 128
highest = lax.Precision.HIGHEST


def split2(x):
    high = x.astype(jnp.bfloat16)
    low = (x - high.astype(jnp.float32)).astype(jnp.bfloat16)
    return high, low


def pack_kernel(dims, row_ref, child_ref, update_ref, pivot_ref, out_ref):
    n, held, planes, extra_rows = dims
    row = row_ref[0]
    width = child_ref.shape[-1]
    lane = lax.broadcasted_iota(jnp.int32, (held, LANES), 1)
    extras = []
    at = 0
    for child in range(2):
        rolled = pltpu.roll(child_ref[0, child], lax.rem(width - row * held, width), 1)
        for plane in range(planes):
            part = rolled[:, plane * LANES : (plane + 1) * LANES]
            if plane == 0:
                part = jnp.where(lane < held, 0.5 * part, part)
            out_ref[0, at : at + held, :] = part
            at += held
        extras.append(rolled[:, planes * LANES : (planes + 1) * LANES])
    extra = jnp.where(row < n // 2, extras[0], extras[1])
    packed = jnp.zeros((extra_rows, LANES), jnp.float32)
    lane = lax.broadcasted_iota(jnp.int32, (extra_rows, LANES), 1)
    for piece in range(held // extra_rows):
        rows = extra[piece * extra_rows : (piece + 1) * extra_rows]
        if piece:
            rows = pltpu.roll(rows, piece * held, 1)
        packed = jnp.where(lane // held == piece, rows, packed)
    out_ref[0, at : at + extra_rows, :] = packed
    at += extra_rows
    out_ref[0, at : at + update_ref.shape[1], :] = update_ref[0]
    at += update_ref.shape[1]
    out_ref[0, at : at + pivot_ref.shape[1], :] = pivot_ref[0]


def front_kernel(dims, map_ref, turned_ref, in_ref, out_ref, pivots_ref, hot_ref, half_ref, sum_ref, aug_ref, coup_ref):
    n, held, planes, extra_rows, update_rows, pivot_rows = dims
    width = map_ref.shape[-1]
    order = sum_ref.shape[0]
    size = aug_ref.shape[0]
    f32, bf16 = jnp.float32, jnp.bfloat16

    def hot(indices):
        count = indices.shape[-1]
        place = lax.broadcasted_iota(jnp.int32, (order, count), 0)
        return jnp.where(place == indices, 1.0, 0.0).astype(bf16)

    last = (((1,), (1,)), ((), ()))
    for child in range(2):
        hot_ref[:, child * width : (child + 1) * width] = hot(map_ref[child : child + 1, :])
        for source in range(n):
            base = child * planes * held
            parts = [
                in_ref[source, base + plane * held : base + (plane + 1) * held, :] for plane in range(planes)
            ]
            columns = planes * LANES
            if (source < n // 2) == (child == 0):
                at = 2 * planes * held
                extra = in_ref[source, at : at + extra_rows, :]
                lane = lax.broadcasted_iota(jnp.int32, (extra_rows, LANES), 1)
                pieces = [
                    jnp.where(lane // held == piece, extra, 0.0) for piece in range(held // extra_rows)
                ]
                parts.append(jnp.concatenate(pieces, axis=0))
                columns += LANES
            high, low = split2(jnp.concatenate(parts, axis=1))
            both = jnp.concatenate([high, low], axis=0)
            spread = lax.dot_general(
                both, hot(turned_ref[source, child : child + 1, :columns]), last, preferred_element_type=f32
            ).astype(bf16)
            at = child * width + source * held
            half_ref[at : at + held, :] = spread[:held]
            half_ref[2 * width + at : 2 * width + at + held, :] = spread[held:]
    for block in range(order // LANES):
        rows = pl.ds(block * LANES, LANES)
        sum_ref[rows, :] = jnp.dot(
            hot_ref[rows, :], half_ref[: 2 * width, :], preferred_element_type=f32
        ) + jnp.dot(hot_ref[rows, :], half_ref[2 * width :, :], preferred_element_type=f32)

    at = 2 * planes * held + extra_rows
    for source in range(n):
        coup_ref[source * update_rows : (source + 1) * update_rows, :] = in_ref[
            source, at : at + update_rows, :
        ]
        aug_ref[source * pivot_rows : (source + 1) * pivot_rows, :size] = in_ref[
            source, at + update_rows : at + update_rows + pivot_rows, :
        ]
    coup_ref[...] += sum_ref[size:, :size] + sum_ref[:size, size:].T
    aug_ref[:, :size] += sum_ref[:size, :size] + sum_ref[:size, :size].T
    square = (size, size)
    aug_ref[:, size:] = jnp.where(
        lax.broadcasted_iota(jnp.int32, square, 0) == lax.broadcasted_iota(jnp.int32, square, 1), 1.0, 0.0
    )

    lanes = lax.broadcasted_iota(jnp.int32, (1, size), 1)
    step = 32
    pivots = jnp.zeros((1, size), f32)
    for start in range(0, size, step):
        rest = size - start
        below = start + lax.broadcasted_iota(jnp.int32, (rest, 1), 0)

        def eliminate(k, pivots, start=start, below=below):
            row = aug_ref[pl.ds(k, 1), :]
            whole = aug_ref[start:, :]
            chosen = lanes == k
            column = jnp.sum(jnp.where(chosen, whole[:, :size], 0.0), axis=1, keepdims=True)
            pivot = jnp.sum(jnp.where(chosen, row[:, :size], 0.0), axis=1, keepdims=True)
            multiplier = jnp.where(below > k, column / pivot, 0.0)
            aug_ref[start:, :] = whole - multiplier * row
            return jnp.where(chosen, pivot, pivots)

        pivots = lax.fori_loop(start, start + step, eliminate, pivots)
    pivots_ref[...] = pivots

    lhat = lax.dot_general(coup_ref[...], aug_ref[:, size:], last, precision=highest, preferred_element_type=f32)
    out_ref[:, :size] = lhat
    coup_ref[...] = lhat / pivots
    for start in range(0, order - size, LANES):
        rows = pl.ds(start, LANES)
        correction = lax.dot_general(
            coup_ref[rows, :], out_ref[:, :size], last, precision=highest, preferred_element_type=f32
        )
        here = size + start
        out_ref[rows, size:] = (
            sum_ref[here : here + LANES, size:] + sum_ref[size:, here : here + LANES].T - correction
        )


def finish_kernel(size, update_ref, back_ref, *refs):
    lhat_ref, schur_ref = refs[-2:]
    lhat_ref[0] = back_ref[0, :, :size]
    schur_ref[0] = update_ref[0, :, size:] + back_ref[0, :, size:]


def local(front_pivot, front_update, child_blocks, child_map):
    f32 = jnp.float32
    n = lax.axis_size("row")
    my_row = lax.axis_index("row")
    fronts, pivot_rows, size = front_pivot.shape
    update_rows, order = front_update.shape[1:]
    held, width = child_blocks.shape[2:]
    per = fronts // n
    planes = width // 2 // LANES
    extra_rows = held * held // LANES
    rows = 2 * planes * held + extra_rows + update_rows + pivot_rows
    row_number = my_row.astype(jnp.int32).reshape(1)

    def pack(turn):
        return pl.pallas_call(
            functools.partial(pack_kernel, (n, held, planes, extra_rows)),
            grid_spec=pltpu.PrefetchScalarGridSpec(
                num_scalar_prefetch=1,
                grid=(n,),
                in_specs=[
                    pl.BlockSpec((1, 2, held, width), lambda g, r: (g * per + turn, 0, 0, 0)),
                    pl.BlockSpec((1, update_rows, size), lambda g, r: (g * per + turn, 0, 0)),
                    pl.BlockSpec((1, pivot_rows, size), lambda g, r: (g * per + turn, 0, 0)),
                ],
                out_specs=pl.BlockSpec((1, rows, LANES), lambda g, r: (g, 0, 0)),
            ),
            out_shape=jax.ShapeDtypeStruct((n, rows, LANES), f32),
            name="pack",
        )(row_number, child_blocks, front_update, front_pivot)

    def whole_front(arrived, turn):
        maps = lax.dynamic_index_in_dim(child_map, my_row * per + turn, 0, keepdims=False)
        twice = jnp.concatenate([maps, maps], axis=1)
        turned = []
        for source in range(n):
            at = source * held
            main = twice[:, at : at + width // 2]
            tail = twice[:, at + width // 2 : at + width // 2 + held]
            turned.append(jnp.concatenate([main] + [tail] * (LANES // held), axis=1))
        turned = jnp.stack(turned)
        return pl.pallas_call(
            functools.partial(front_kernel, (n, held, planes, extra_rows, update_rows, pivot_rows)),
            out_shape=(
                jax.ShapeDtypeStruct((order - size, order), f32),
                jax.ShapeDtypeStruct((1, size), f32),
            ),
            scratch_shapes=[
                pltpu.VMEM((order, 2 * width), jnp.bfloat16),
                pltpu.VMEM((4 * width, order), jnp.bfloat16),
                pltpu.VMEM((order, order), f32),
                pltpu.VMEM((size, 2 * size), f32),
                pltpu.VMEM((order - size, size), f32),
            ],
            name="front",
        )(maps, turned, arrived)

    def finish(back, turn, before):
        aliases = {2: 0, 3: 1} if before else {}
        anywhere = [pl.BlockSpec(memory_space=pl.ANY)] * len(before)
        return pl.pallas_call(
            functools.partial(finish_kernel, size),
            grid=(n,),
            in_specs=[
                pl.BlockSpec((1, update_rows, order), lambda g: (g * per + turn, 0, 0)),
                pl.BlockSpec((1, update_rows, order), lambda g: (g, 0, 0)),
            ]
            + anywhere,
            out_specs=(
                pl.BlockSpec((1, update_rows, size), lambda g: (g * per + turn, 0, 0)),
                pl.BlockSpec((1, update_rows, order - size), lambda g: (g * per + turn, 0, 0)),
            ),
            out_shape=(
                jax.ShapeDtypeStruct((fronts, update_rows, size), f32),
                jax.ShapeDtypeStruct((fronts, update_rows, order - size), f32),
            ),
            input_output_aliases=aliases,
            name="finish",
        )(front_update, back, *before)

    exchange = functools.partial(lax.all_to_all, axis_name="row", split_axis=0, concat_axis=0, tiled=True)
    arrived = [exchange(pack(turn)) for turn in range(per)]
    negatives = jnp.zeros((), f32)
    backs = []
    for turn in range(per):
        rows_out, pivots = whole_front(arrived[turn], turn)
        backs.append(exchange(rows_out.reshape(n, update_rows, order)))
        negatives = negatives + jnp.sum(jnp.where(pivots < 0.0, 1.0, 0.0))
    done = ()
    for turn in range(per):
        done = finish(backs[turn], turn, done)
    lhat, schur = done
    total = lax.psum(negatives, ("row", "col"))
    negative_share = total / (fronts * lax.axis_size("col") * size)
    return (lhat, schur, negative_share)


def solution(mesh):
    in_specs = (
        P("col", "row", None),
        P("col", "row", None),
        P("col", None, "row", None),
        P("col", None, None),
    )
    out_specs = (P("col", "row", None), P("col", "row", None), P())
    return jax.shard_map(local, mesh=mesh, in_specs=in_specs, out_specs=out_specs, check_vma=False)
```

```python
import functools

import jax
import jax.numpy as jnp
from jax import lax
from jax.experimental import pallas as pl
from jax.experimental.pallas import tpu as pltpu
from jax.sharding import PartitionSpec as P

LANES = 128
highest = lax.Precision.HIGHEST


def split2(x):
    high = x.astype(jnp.bfloat16)
    low = (x - high.astype(jnp.float32)).astype(jnp.bfloat16)
    return high, low


def pack_kernel(dims, row_ref, child_ref, update_ref, pivot_ref, out_ref):
    n, held, extra_rows = dims
    row = row_ref[0]
    half = n // 2
    span = half * held
    place = lax.rem(row, half)
    lane = lax.broadcasted_iota(jnp.int32, (held, LANES), 1)
    lane_extra = lax.broadcasted_iota(jnp.int32, (extra_rows, LANES), 1)
    for front in range(child_ref.shape[0]):
        extras = []
        at = 0
        for child in range(2):
            rolled = pltpu.roll(child_ref[front, 0, child], lax.rem(span - place * held, span), 1)
            near = rolled[:, :LANES]
            out_ref[front, at : at + held, :] = jnp.where(lane < held, 0.5 * near, near)
            at += held
            extras.append(rolled[:, LANES:])
        extra = jnp.where(place < half // 2, extras[0], extras[1])
        packed = extra[:extra_rows]
        for piece in range(1, held // extra_rows):
            rows = pltpu.roll(extra[piece * extra_rows : (piece + 1) * extra_rows], piece * held, 1)
            packed = jnp.where(lane_extra // held == piece, rows, packed)
        out_ref[front, at : at + extra_rows, :] = packed
        at += extra_rows
        out_ref[front, at : at + update_ref.shape[2], :] = update_ref[front, 0]
        at += update_ref.shape[2]
        out_ref[front, at : at + pivot_ref.shape[2], :] = pivot_ref[front, 0]


def inner_kernel(dims, row_ref, child_ref, *refs):
    n, per, turn, span = dims
    outs, sem = refs[:-1], refs[-1]
    row = row_ref[0]
    half = n // 2
    columns = pl.ds(pl.multiple_of((1 - row // half) * span, LANES), span)
    copies = []
    for flip, out_ref in enumerate(outs):
        front = (row ^ flip) * per + turn
        copies.append(pltpu.make_async_copy(child_ref.at[front, :, :, columns], out_ref, sem.at[flip]))
    for copy in copies:
        copy.start()
    for copy in copies:
        copy.wait()


def front_kernel(dims, row_ref, map_ref, in_ref, *refs):
    n, held, extra_rows, update_rows, pivot_rows = dims
    half = n // 2
    inner_refs = refs[:half]
    out_ref, pivots_ref, hot_ref, half_ref, sum_ref, aug_ref, coup_ref = refs[half:]
    row = row_ref[0]
    width = map_ref.shape[-1]
    span = half * held
    order = sum_ref.shape[0]
    size = aug_ref.shape[0]
    f32, bf16 = jnp.float32, jnp.bfloat16

    def hot(indices):
        place = lax.broadcasted_iota(jnp.int32, (order, indices.shape[-1]), 0)
        return jnp.where(place == indices, 1.0, 0.0).astype(bf16)

    last = (((1,), (1,)), ((), ()))

    def spread(values, table):
        high, low = split2(values)
        both = jnp.concatenate([high, low], axis=0)
        return lax.dot_general(both, table, last, preferred_element_type=f32).astype(bf16)

    lane = lax.broadcasted_iota(jnp.int32, (extra_rows, LANES), 1)
    lane8 = lax.broadcasted_iota(jnp.int32, (8, LANES), 1)
    pieces = held // extra_rows
    for child in range(2):
        indices = map_ref[0, child : child + 1, :]
        hot_ref[:, child * width : (child + 1) * width] = hot(indices)
        for source in range(n):
            place = source % half
            start = source // half * span
            turned = jnp.broadcast_to(indices[:, start : start + span], (8, span))
            if place:
                turned = pltpu.roll(turned, span - place * held, 1)
            values = in_ref[source, child * held : (child + 1) * held, :]
            table = turned[:1, :LANES]
            if (place < half // 2) == (child == 0):
                extra = in_ref[source, 2 * held : 2 * held + extra_rows, :]
                values = jnp.concatenate(
                    [
                        values,
                        jnp.concatenate(
                            [jnp.where(lane // held == piece, extra, 0.0) for piece in range(pieces)], axis=0
                        ),
                    ],
                    axis=1,
                )
                far = turned[:, LANES : 2 * LANES]
                tiled = far
                for piece in range(1, pieces):
                    tiled = jnp.where(lane8 // held == piece, pltpu.roll(far, piece * held, 1), tiled)
                table = jnp.concatenate([table, tiled[:1]], axis=1)
            moved = spread(values, hot(table))
            at = child * width + source * held
            half_ref[at : at + held, :] = moved[:held]
            half_ref[2 * width + at : 2 * width + at + held, :] = moved[held:]
        other = hot(jnp.where(row // half == 0, indices[:, span:], indices[:, :span]))
        for flip in range(half):
            moved = spread(inner_refs[flip][child], other)
            at = pl.multiple_of(child * width + (row ^ flip) * held, held)
            half_ref[pl.ds(at, held), :] += moved[:held]
            half_ref[pl.ds(2 * width + at, held), :] += moved[held:]
    for block in range(order // LANES):
        rows = pl.ds(block * LANES, LANES)
        sum_ref[rows, :] = jnp.dot(
            hot_ref[rows, :], half_ref[: 2 * width, :], preferred_element_type=f32
        ) + jnp.dot(hot_ref[rows, :], half_ref[2 * width :, :], preferred_element_type=f32)

    at = 2 * held + extra_rows
    for source in range(n):
        coup_ref[source * update_rows : (source + 1) * update_rows, :] = in_ref[
            source, at : at + update_rows, :
        ]
        aug_ref[source * pivot_rows : (source + 1) * pivot_rows, :size] = in_ref[
            source, at + update_rows : at + update_rows + pivot_rows, :
        ]
    coup_ref[...] += sum_ref[size:, :size] + sum_ref[:size, size:].T
    aug_ref[:, :size] += sum_ref[:size, :size] + sum_ref[:size, :size].T
    square = (size, size)
    aug_ref[:, size:] = jnp.where(
        lax.broadcasted_iota(jnp.int32, square, 0) == lax.broadcasted_iota(jnp.int32, square, 1), 1.0, 0.0
    )

    lanes = lax.broadcasted_iota(jnp.int32, (1, size), 1)
    step = 32
    pivots = jnp.zeros((1, size), f32)
    for start in range(0, size, step):
        rest = size - start
        below = start + lax.broadcasted_iota(jnp.int32, (rest, 1), 0)

        def eliminate(k, pivots, start=start, below=below):
            row = aug_ref[pl.ds(k, 1), :]
            whole = aug_ref[start:, :]
            chosen = lanes == k
            column = jnp.sum(jnp.where(chosen, whole[:, :size], 0.0), axis=1, keepdims=True)
            pivot = jnp.sum(jnp.where(chosen, row[:, :size], 0.0), axis=1, keepdims=True)
            multiplier = jnp.where(below > k, column / pivot, 0.0)
            aug_ref[start:, :] = whole - multiplier * row
            return jnp.where(chosen, pivot, pivots)

        pivots = lax.fori_loop(start, start + step, eliminate, pivots)
    pivots_ref[...] = pivots

    lhat = lax.dot_general(coup_ref[...], aug_ref[:, size:], last, precision=highest, preferred_element_type=f32)
    out_ref[:, :size] = lhat
    coup_ref[...] = lhat / pivots
    for start in range(0, order - size, LANES):
        rows = pl.ds(start, LANES)
        correction = lax.dot_general(
            coup_ref[rows, :], out_ref[:, :size], last, precision=highest, preferred_element_type=f32
        )
        here = size + start
        out_ref[rows, size:] = (
            sum_ref[here : here + LANES, size:] + sum_ref[size:, here : here + LANES].T - correction
        )


def finish_kernel(size, update_ref, back_ref, *refs):
    lhat_ref, schur_ref = refs[-2:]
    count = update_ref.shape[0]
    rows = pl.ds(pl.program_id(0) * count, count)
    lhat_ref[:, 0] = back_ref[rows, :, :size]
    schur_ref[:, 0] = update_ref[:, 0, :, size:] + back_ref[rows, :, size:]


def local(front_pivot, front_update, child_blocks, child_map):
    f32 = jnp.float32
    n = lax.axis_size("row")
    half = n // 2
    my_row = lax.axis_index("row")
    fronts, pivot_rows, size = front_pivot.shape
    update_rows, order = front_update.shape[1:]
    held, width = child_blocks.shape[2:]
    per = fronts // n
    span = half * held
    extra_rows = held * held // LANES
    rows = 2 * held + extra_rows + update_rows + pivot_rows
    row_number = my_row.astype(jnp.int32).reshape(1)
    dims = (n, held, extra_rows)
    group = n // 2
    vmem = pl.BlockSpec(memory_space=pltpu.VMEM)
    whole = pl.BlockSpec(memory_space=pl.ANY)

    def pack(turn):
        return pl.pallas_call(
            functools.partial(pack_kernel, dims),
            grid_spec=pltpu.PrefetchScalarGridSpec(
                num_scalar_prefetch=1,
                grid=(n // group,),
                in_specs=[
                    pl.BlockSpec((group, 1, 2, held, span), lambda g, r: (g, turn, 0, 0, r[0] // half)),
                    pl.BlockSpec((group, 1, update_rows, size), lambda g, r: (g, turn, 0, 0)),
                    pl.BlockSpec((group, 1, pivot_rows, size), lambda g, r: (g, turn, 0, 0)),
                ],
                out_specs=pl.BlockSpec((group, rows, LANES), lambda g, r: (g, 0, 0)),
            ),
            out_shape=jax.ShapeDtypeStruct((n, rows, LANES), f32),
            name="pack",
        )(
            row_number,
            child_blocks.reshape(n, per, 2, held, width),
            front_update.reshape(n, per, update_rows, order),
            front_pivot.reshape(n, per, pivot_rows, size),
        )

    def inner(turn):
        return pl.pallas_call(
            functools.partial(inner_kernel, (n, per, turn, span)),
            in_specs=[pl.BlockSpec(memory_space=pltpu.SMEM), whole],
            out_specs=[whole] * half,
            out_shape=[jax.ShapeDtypeStruct((2, held, span), f32)] * half,
            scratch_shapes=[pltpu.SemaphoreType.DMA((half,))],
            name="inner",
        )(row_number, child_blocks)

    def whole_front(arrived, inners, turn):
        return pl.pallas_call(
            functools.partial(front_kernel, dims + (update_rows, pivot_rows)),
            grid_spec=pltpu.PrefetchScalarGridSpec(
                num_scalar_prefetch=1,
                grid=(1,),
                in_specs=[pl.BlockSpec((1, 2, width), lambda g, r: (r[0] * per + turn, 0, 0))]
                + [vmem] * (half + 1),
                out_specs=(vmem, vmem),
                scratch_shapes=[
                    pltpu.VMEM((order, 2 * width), jnp.bfloat16),
                    pltpu.VMEM((4 * width, order), jnp.bfloat16),
                    pltpu.VMEM((order, order), f32),
                    pltpu.VMEM((size, 2 * size), f32),
                    pltpu.VMEM((order - size, size), f32),
                ],
            ),
            out_shape=(
                jax.ShapeDtypeStruct((order - size, order), f32),
                jax.ShapeDtypeStruct((1, size), f32),
            ),
            name="front",
        )(row_number, child_map, arrived, *inners)

    def finish(back, turn, before):
        aliases = {2: 0, 3: 1} if before else {}
        group = 2
        place = lambda g: (g, turn, 0, 0)
        return pl.pallas_call(
            functools.partial(finish_kernel, size),
            grid=(n // group,),
            in_specs=[pl.BlockSpec((group, 1, update_rows, order), place), vmem] + [whole] * len(before),
            out_specs=(
                pl.BlockSpec((group, 1, update_rows, size), place),
                pl.BlockSpec((group, 1, update_rows, order - size), place),
            ),
            out_shape=(
                jax.ShapeDtypeStruct((n, per, update_rows, size), f32),
                jax.ShapeDtypeStruct((n, per, update_rows, order - size), f32),
            ),
            input_output_aliases=aliases,
            name="finish",
        )(front_update.reshape(n, per, update_rows, order), back, *before)

    exchange = functools.partial(lax.all_to_all, axis_name="row", split_axis=0, concat_axis=0, tiled=True)

    def near(parts):
        return [parts[0]] + [
            lax.ppermute(parts[flip], "row", [(i, i ^ flip) for i in range(n)]) for flip in range(1, half)
        ]

    packed = [pack(turn) for turn in range(per)]
    inners = [near(inner(turn)) for turn in range(per)]
    arrived = [exchange(packed[turn]) for turn in range(per)]
    total = jnp.zeros((), f32)
    backs = []
    for turn in range(per):
        rows_out, pivots = whole_front(arrived[turn], inners[turn], turn)
        total = total + jnp.sum(jnp.where(pivots < 0.0, 1.0, 0.0))
        if turn == per - 1:
            total = lax.psum(total, ("row", "col"))
            rows_out, total = lax.optimization_barrier((rows_out, total))
        backs.append(exchange(rows_out.reshape(n, update_rows, order)))
    done = ()
    for turn in range(per):
        done = finish(backs[turn], turn, done)
    lhat, schur = done
    negative_share = total / (fronts * lax.axis_size("col") * size)
    return (
        lhat.reshape(fronts, update_rows, size),
        schur.reshape(fronts, update_rows, order - size),
        negative_share,
    )


def solution(mesh):
    in_specs = (
        P("col", "row", None),
        P("col", "row", None),
        P("col", None, "row", None),
        P("col", None, None),
    )
    out_specs = (P("col", "row", None), P("col", "row", None), P())
    return jax.shard_map(local, mesh=mesh, in_specs=in_specs, out_specs=out_specs, check_vma=False)
```

```python
import functools

import jax
import jax.numpy as jnp
from jax import lax
from jax.experimental import pallas as pl
from jax.experimental.pallas import tpu as pltpu
from jax.sharding import PartitionSpec as P


LANES = 128
highest = lax.Precision.HIGHEST


def split2(x):
    high = x.astype(jnp.bfloat16)
    low = (x - high.astype(jnp.float32)).astype(jnp.bfloat16)
    return high, low


def pack_kernel(dims, row_ref, child_ref, update_ref, pivot_ref, out_ref):
    n, held, extra_rows = dims
    row = row_ref[0]
    half = n // 2
    span = half * held
    place = lax.rem(row, half)
    lane = lax.broadcasted_iota(jnp.int32, (held, LANES), 1)
    lane_extra = lax.broadcasted_iota(jnp.int32, (extra_rows, LANES), 1)
    for front in range(child_ref.shape[0]):
        extras = []
        at = 0
        for child in range(2):
            rolled = pltpu.roll(child_ref[front, 0, child], lax.rem(span - place * held, span), 1)
            near = rolled[:, :LANES]
            out_ref[front, at : at + held, :] = jnp.where(lane < held, 0.5 * near, near)
            at += held
            extras.append(rolled[:, LANES:])
        extra = jnp.where(place < half // 2, extras[0], extras[1])
        packed = extra[:extra_rows]
        for piece in range(1, held // extra_rows):
            rows = pltpu.roll(extra[piece * extra_rows : (piece + 1) * extra_rows], piece * held, 1)
            packed = jnp.where(lane_extra // held == piece, rows, packed)
        out_ref[front, at : at + extra_rows, :] = packed
        at += extra_rows
        out_ref[front, at : at + update_ref.shape[2], :] = update_ref[front, 0]
        at += update_ref.shape[2]
        out_ref[front, at : at + pivot_ref.shape[2], :] = pivot_ref[front, 0]


def inner_kernel(*refs):
    count = (len(refs) - 1) // 2
    for in_ref, out_ref in zip(refs[1 : 1 + count], refs[1 + count :]):
        out_ref[...] = in_ref[0]


def assemble(dims, row, map_ref, in_ref, inner_refs, hot_ref, half_ref, sum_ref, aug_ref, coup_ref):
    n, held, extra_rows, update_rows, pivot_rows = dims
    half = n // 2
    width = map_ref.shape[-1]
    span = half * held
    order = sum_ref.shape[0]
    size = aug_ref.shape[0]
    f32, bf16 = jnp.float32, jnp.bfloat16

    def hot(indices):
        place = lax.broadcasted_iota(jnp.int32, (order, indices.shape[-1]), 0)
        return jnp.where(place == indices, 1.0, 0.0).astype(bf16)

    last = (((1,), (1,)), ((), ()))

    def spread(values, table):
        high, low = split2(values)
        both = jnp.concatenate([high, low], axis=0)
        return lax.dot_general(both, table, last, preferred_element_type=f32).astype(bf16)

    lane = lax.broadcasted_iota(jnp.int32, (extra_rows, LANES), 1)
    lane8 = lax.broadcasted_iota(jnp.int32, (8, LANES), 1)
    pieces = held // extra_rows
    for child in range(2):
        indices = map_ref[0, child : child + 1, :]
        hot_ref[:, child * width : (child + 1) * width] = hot(indices)
        for source in range(n):
            place = source % half
            start = source // half * span
            turned = jnp.broadcast_to(indices[:, start : start + span], (8, span))
            if place:
                turned = pltpu.roll(turned, span - place * held, 1)
            values = in_ref[source, child * held : (child + 1) * held, :]
            table = turned[:1, :LANES]
            if (place < half // 2) == (child == 0):
                extra = in_ref[source, 2 * held : 2 * held + extra_rows, :]
                values = jnp.concatenate(
                    [
                        values,
                        jnp.concatenate(
                            [jnp.where(lane // held == piece, extra, 0.0) for piece in range(pieces)], axis=0
                        ),
                    ],
                    axis=1,
                )
                far = turned[:, LANES : 2 * LANES]
                tiled = far
                for piece in range(1, pieces):
                    tiled = jnp.where(lane8 // held == piece, pltpu.roll(far, piece * held, 1), tiled)
                table = jnp.concatenate([table, tiled[:1]], axis=1)
            moved = spread(values, hot(table))
            at = child * width + source * held
            half_ref[at : at + held, :] = moved[:held]
            half_ref[2 * width + at : 2 * width + at + held, :] = moved[held:]
        other = hot(jnp.where(row // half == 0, indices[:, span:], indices[:, :span]))
        for flip in range(half):
            moved = spread(inner_refs[flip][child], other)
            at = pl.multiple_of(child * width + (row ^ flip) * held, held)
            half_ref[pl.ds(at, held), :] += moved[:held]
            half_ref[pl.ds(2 * width + at, held), :] += moved[held:]
    for block in range(order // LANES):
        rows = pl.ds(block * LANES, LANES)
        sum_ref[rows, :] = jnp.dot(
            hot_ref[rows, :], half_ref[: 2 * width, :], preferred_element_type=f32
        ) + jnp.dot(hot_ref[rows, :], half_ref[2 * width :, :], preferred_element_type=f32)

    at = 2 * held + extra_rows
    for source in range(n):
        coup_ref[source * update_rows : (source + 1) * update_rows, :] = in_ref[
            source, at : at + update_rows, :
        ]
        aug_ref[source * pivot_rows : (source + 1) * pivot_rows, :size] = in_ref[
            source, at + update_rows : at + update_rows + pivot_rows, :
        ]
    coup_ref[...] += sum_ref[size:, :size] + sum_ref[:size, size:].T
    aug_ref[:, :size] += sum_ref[:size, :size] + sum_ref[:size, :size].T
    square = (size, size)
    aug_ref[:, size:] = jnp.where(
        lax.broadcasted_iota(jnp.int32, square, 0) == lax.broadcasted_iota(jnp.int32, square, 1), 1.0, 0.0
    )


def eliminate(aug_ref):
    size = aug_ref.shape[0]
    lanes = lax.broadcasted_iota(jnp.int32, (1, size), 1)
    step = 32
    pivots = jnp.zeros((1, size), jnp.float32)
    for start in range(0, size, step):
        rest = size - start
        below = start + lax.broadcasted_iota(jnp.int32, (rest, 1), 0)

        def one(k, pivots, start=start, below=below):
            row = aug_ref[pl.ds(k, 1), :]
            whole = aug_ref[start:, :]
            chosen = lanes == k
            column = jnp.sum(jnp.where(chosen, whole[:, :size], 0.0), axis=1, keepdims=True)
            pivot = jnp.sum(jnp.where(chosen, row[:, :size], 0.0), axis=1, keepdims=True)
            multiplier = jnp.where(below > k, column / pivot, 0.0)
            aug_ref[start:, :] = whole - multiplier * row
            return jnp.where(chosen, pivot, pivots)

        pivots = lax.fori_loop(start, start + step, one, pivots)
    return pivots


def trailing(sum_ref, size, start):
    here = size + start
    return sum_ref[here : here + LANES, size:] + sum_ref[size:, here : here + LANES].T


LAST = (((1,), (1,)), ((), ()))


def update(out_ref, coup_ref, inverse, pivots, trailing_rows):
    size = inverse.shape[0]
    f32 = jnp.float32
    lhat = lax.dot_general(coup_ref[...], inverse, LAST, precision=highest, preferred_element_type=f32)
    out_ref[:, :size] = lhat
    coup_ref[...] = lhat / pivots
    for start in range(0, out_ref.shape[0], LANES):
        rows = pl.ds(start, LANES)
        correction = lax.dot_general(
            coup_ref[rows, :], out_ref[:, :size], LAST, precision=highest, preferred_element_type=f32
        )
        out_ref[rows, size:] = trailing_rows(start) - correction


def front_kernel(dims, row_ref, map_ref, in_ref, *refs):
    half = dims[0] // 2
    out_ref, pivots_ref, hot_ref, half_ref, sum_ref, aug_ref, coup_ref = refs[half:]
    assemble(dims, row_ref[0], map_ref, in_ref, refs[:half], hot_ref, half_ref, sum_ref, aug_ref, coup_ref)
    size = aug_ref.shape[0]
    pivots = eliminate(aug_ref)
    pivots_ref[...] = pivots
    update(out_ref, coup_ref, aug_ref[:, size:], pivots, functools.partial(trailing, sum_ref, size))


def factor_kernel(dims, row_ref, map_ref, in_ref, *refs):
    half = dims[0] // 2
    trail_ref, coup_ref, inverse_ref, pivots_ref, hot_ref, half_ref, sum_ref, aug_ref = refs[half:]
    assemble(dims, row_ref[0], map_ref, in_ref, refs[:half], hot_ref, half_ref, sum_ref, aug_ref, coup_ref)
    size = aug_ref.shape[0]
    pivots_ref[...] = eliminate(aug_ref)
    inverse_ref[...] = aug_ref[:, size:]
    for start in range(0, trail_ref.shape[0], LANES):
        trail_ref[pl.ds(start, LANES), :] = trailing(sum_ref, size, start)


def schur_kernel(row_ref, count_ref, trail_ref, coup_in_ref, inverse_ref, pivots_ref, *refs):
    out_refs = refs[:-2]
    full_ref, coup_ref = refs[-2:]
    coup_ref[...] = coup_in_ref[...]
    update(
        full_ref, coup_ref, inverse_ref[...], pivots_ref[...], lambda start: trail_ref[pl.ds(start, LANES), :]
    )
    update_rows, order = out_refs[0].shape
    size = inverse_ref.shape[0]
    shape = (8, order)
    first = lax.broadcasted_iota(jnp.int32, shape, 0)
    second = lax.broadcasted_iota(jnp.int32, shape, 1)
    for flip, out_ref in enumerate(out_refs):
        home = row_ref[0] ^ flip
        at = pl.multiple_of(home * update_rows, 8)
        out_ref[...] = full_ref[pl.ds(at, update_rows), :]
        chosen = (first == 1) & (second == size + at)
        out_ref[:8, :] = jnp.where(chosen, count_ref[0], full_ref[pl.ds(at, 8), :])


def finish_kernel(size, update_ref, back_ref, *refs):
    lhat_ref, schur_ref = refs[-2:]
    count = update_ref.shape[0]
    rows = pl.ds(pl.program_id(0) * count, count)
    lhat_ref[:, 0] = back_ref[rows, :, :size]
    schur_ref[:, 0] = update_ref[:, 0, :, size:] + back_ref[rows, :, size:]


def last_kernel(size, count, row_ref, update_ref, *refs):
    back_refs, seen_ref = refs[:count], refs[count]
    lhat_ref, schur_ref, total_ref = refs[-3:]
    step = pl.program_id(0)
    update_rows, order = back_refs[0].shape
    shape = (8, order - size)
    first = lax.broadcasted_iota(jnp.int32, shape, 0)
    second = lax.broadcasted_iota(jnp.int32, shape, 1)
    at = row_ref[0] * update_rows

    @pl.when(step == 0)
    def _():
        total_ref[...] = seen_ref[...]

    for which in range(count):

        @pl.when(step == which)
        def _(which=which):
            back = back_refs[which]
            lhat_ref[0] = back[:, :size]
            schur_ref[0] = update_ref[0, :, size:] + back[:, size:]
            head = back[:8, size:]
            marked = (first == 1) & (second == at)
            twin = jnp.sum(jnp.where((first == 0) & (second == at + 1), head, 0.0))
            total_ref[...] += jnp.sum(jnp.where(marked, head, 0.0))
            schur_ref[0, :8, :] = update_ref[0, :8, size:] + jnp.where(marked, twin, head)


def local_body(front_pivot, front_update, child_blocks, child_map):
    f32 = jnp.float32
    n = lax.axis_size("row")
    half = n // 2
    my_row = lax.axis_index("row")
    fronts, pivot_rows, size = front_pivot.shape
    update_rows, order = front_update.shape[1:]
    held, width = child_blocks.shape[2:]
    per = fronts // n
    span = half * held
    extra_rows = held * held // LANES
    rows = 2 * held + extra_rows + update_rows + pivot_rows
    row_number = my_row.astype(jnp.int32).reshape(1)
    dims = (n, held, extra_rows)
    group = n // 2
    vmem = pl.BlockSpec(memory_space=pltpu.VMEM)
    whole = pl.BlockSpec(memory_space=pl.ANY)
    updates = front_update.reshape(n, per, update_rows, order)
    flat = jax.ShapeDtypeStruct

    def pack(turn):
        return pl.pallas_call(
            functools.partial(pack_kernel, dims),
            grid_spec=pltpu.PrefetchScalarGridSpec(
                num_scalar_prefetch=1,
                grid=(n // group,),
                in_specs=[
                    pl.BlockSpec((group, 1, 2, held, span), lambda g, r: (g, turn, 0, 0, r[0] // half)),
                    pl.BlockSpec((group, 1, update_rows, size), lambda g, r: (g, turn, 0, 0)),
                    pl.BlockSpec((group, 1, pivot_rows, size), lambda g, r: (g, turn, 0, 0)),
                ],
                out_specs=pl.BlockSpec((group, rows, LANES), lambda g, r: (g, 0, 0)),
            ),
            out_shape=flat((n, rows, LANES), f32),
            name="pack",
        )(
            row_number,
            child_blocks.reshape(n, per, 2, held, width),
            updates,
            front_pivot.reshape(n, per, pivot_rows, size),
        )

    def inner(turn):
        def spec(flip):
            return pl.BlockSpec(
                (1, 2, held, span), lambda g, r: ((r[0] ^ flip) * per + turn, 0, 0, 1 - r[0] // half)
            )

        return pl.pallas_call(
            inner_kernel,
            grid_spec=pltpu.PrefetchScalarGridSpec(
                num_scalar_prefetch=1,
                grid=(1,),
                in_specs=[spec(flip) for flip in range(half)],
                out_specs=[vmem] * half,
            ),
            out_shape=[flat((2, held, span), f32)] * half,
            name="inner",
        )(row_number, *[child_blocks] * half)

    def from_arrived(kernel, arrived, inners, turn, outs, scratch):
        return pl.pallas_call(
            functools.partial(kernel, dims + (update_rows, pivot_rows)),
            grid_spec=pltpu.PrefetchScalarGridSpec(
                num_scalar_prefetch=1,
                grid=(1,),
                in_specs=[pl.BlockSpec((1, 2, width), lambda g, r: (r[0] * per + turn, 0, 0))]
                + [vmem] * (half + 1),
                out_specs=(vmem,) * len(outs),
                scratch_shapes=[
                    pltpu.VMEM((order, 2 * width), jnp.bfloat16),
                    pltpu.VMEM((4 * width, order), jnp.bfloat16),
                    pltpu.VMEM((order, order), f32),
                    pltpu.VMEM((size, 2 * size), f32),
                ]
                + scratch,
            ),
            out_shape=tuple(flat(shape, f32) for shape in outs),
            name="front",
        )(row_number, child_map, arrived, *inners)

    def whole_front(arrived, inners, turn):
        outs = [(order - size, order), (1, size)]
        scratch = [pltpu.VMEM((order - size, size), f32)]
        return from_arrived(front_kernel, arrived, inners, turn, outs, scratch)

    def factored(arrived, inners, turn):
        outs = [(order - size, order - size), (order - size, size), (size, size), (1, size)]
        return from_arrived(factor_kernel, arrived, inners, turn, outs, [])

    def schur_rows(count, parts):
        smem = pl.BlockSpec(memory_space=pltpu.SMEM)
        return pl.pallas_call(
            schur_kernel,
            in_specs=[smem, smem] + [vmem] * 4,
            out_specs=[vmem] * n,
            out_shape=[flat((update_rows, order), f32)] * n,
            scratch_shapes=[pltpu.VMEM((order - size, order), f32), pltpu.VMEM((order - size, size), f32)],
            name="schur",
        )(row_number, count.reshape(1), *parts)

    def finish(back, turn, before):
        aliases = {2: 0, 3: 1} if before else {}
        group = 2
        place = lambda g: (g, turn, 0, 0)
        return pl.pallas_call(
            functools.partial(finish_kernel, size),
            grid=(n // group,),
            in_specs=[pl.BlockSpec((group, 1, update_rows, order), place), vmem] + [whole] * len(before),
            out_specs=(
                pl.BlockSpec((group, 1, update_rows, size), place),
                pl.BlockSpec((group, 1, update_rows, order - size), place),
            ),
            out_shape=(
                flat((n, per, update_rows, size), f32),
                flat((n, per, update_rows, order - size), f32),
            ),
            input_output_aliases=aliases,
            name="finish",
        )(updates, back, *before)

    def last(backs, flips, turn, before, seen):
        count = len(backs)
        place = lambda g, r: ((r[0] ^ (flips[0] + g)) * per + turn, 0, 0)
        before = [part.reshape(fronts, update_rows, -1) for part in before]
        aliases = {3 + count: 0, 4 + count: 1} if before else {}
        return pl.pallas_call(
            functools.partial(last_kernel, size, count),
            grid_spec=pltpu.PrefetchScalarGridSpec(
                num_scalar_prefetch=1,
                grid=(count,),
                in_specs=[pl.BlockSpec((1, update_rows, order), place)]
                + [vmem] * (count + 1)
                + [whole] * len(before),
                out_specs=(
                    pl.BlockSpec((1, update_rows, size), place),
                    pl.BlockSpec((1, update_rows, order - size), place),
                    pl.BlockSpec((1, size), lambda g, r: (0, 0)),
                ),
            ),
            out_shape=(
                flat((fronts, update_rows, size), f32),
                flat((fronts, update_rows, order - size), f32),
                flat((1, size), f32),
            ),
            input_output_aliases=aliases,
            name="last",
        )(row_number, front_update, *backs, seen, *before)

    exchange = functools.partial(lax.all_to_all, axis_name="row", split_axis=0, concat_axis=0, tiled=True)

    def send(part, flip):
        return lax.ppermute(part, "row", [(i, i ^ flip) for i in range(n)])

    arrived, inners = [], []
    for turn in range(per):
        packed = pack(turn)
        arrived.append(exchange(packed))
        parts = inner(turn)
        inners.append([parts[0]] + [send(parts[flip], flip) for flip in range(1, half)])
    total = jnp.zeros((), f32)
    backs = []
    for turn in range(per - 1):
        rows_out, pivots = whole_front(arrived[turn], inners[turn], turn)
        total = total + jnp.sum(jnp.where(pivots < 0.0, 1.0, 0.0))
        backs.append(exchange(rows_out.reshape(n, update_rows, order)))
    turn = per - 1
    parts = factored(arrived[turn], inners[turn], turn)
    total = lax.psum(total + jnp.sum(jnp.where(parts[3] < 0.0, 1.0, 0.0)), "col")
    homes = schur_rows(total, parts)
    homes = [homes[0]] + [send(homes[flip], flip) for flip in range(1, n)]
    done = ()
    for turn in range(per - 1):
        done = finish(backs[turn], turn, done)
    seen = jnp.zeros((1, size), f32)
    for begin in (0, half):
        flips = range(begin, begin + half)
        lhat, schur, seen = last([homes[flip] for flip in flips], flips, per - 1, done, seen)
        done = (lhat, schur)
    negative_share = seen[0, 0] / (fronts * lax.axis_size("col") * size)
    return (lhat, schur, negative_share)


def solution(mesh):
    in_specs = (
        P("col", "row", None),
        P("col", "row", None),
        P("col", None, "row", None),
        P("col", None, None),
    )
    out_specs = (P("col", "row", None), P("col", "row", None), P())
    return jax.shard_map(local_body, mesh=mesh, in_specs=in_specs, out_specs=out_specs, check_vma=False)
```

```python
import functools

import jax
import jax.numpy as jnp
from jax import lax
from jax.experimental import pallas as pl
from jax.experimental.pallas import tpu as pltpu
from jax.sharding import PartitionSpec as P


LANES = 128
highest = lax.Precision.HIGHEST


def split2(x):
    high = x.astype(jnp.bfloat16)
    low = (x - high.astype(jnp.float32)).astype(jnp.bfloat16)
    return high, low


def fill(dims, row, children, coupling, pivots, out_ref):
    n, held, extra_rows = dims
    half = n // 2
    span = half * held
    place = lax.rem(row, half)
    lane = lax.broadcasted_iota(jnp.int32, (held, LANES), 1)
    lane_extra = lax.broadcasted_iota(jnp.int32, (extra_rows, LANES), 1)
    extras = []
    at = 0
    for child in range(2):
        rolled = pltpu.roll(children[child], lax.rem(span - place * held, span), 1)
        near = rolled[:, :LANES]
        out_ref[at : at + held, :] = jnp.where(lane < held, 0.5 * near, near)
        at += held
        extras.append(rolled[:, LANES:])
    extra = jnp.where(place < half // 2, extras[0], extras[1])
    packed = extra[:extra_rows]
    for piece in range(1, held // extra_rows):
        rows = pltpu.roll(extra[piece * extra_rows : (piece + 1) * extra_rows], piece * held, 1)
        packed = jnp.where(lane_extra // held == piece, rows, packed)
    for part in (packed, coupling, pivots):
        out_ref[at : at + part.shape[0], :] = part
        at += part.shape[0]
    return at


def pack_kernel(dims, row_ref, child_ref, update_ref, pivot_ref, out_ref):
    for front in range(child_ref.shape[0]):
        fill(
            dims, row_ref[0], child_ref.at[front, 0], update_ref[front, 0], pivot_ref[front, 0], out_ref.at[front]
        )


def part_kernel(dims, count, row_ref, *refs):
    inputs, outs = refs[:-count], refs[-count:]
    groups = [inputs[at : at + count] for at in range(0, len(inputs), count)]
    for which, out_ref in enumerate(outs):
        children, coupling, pivots = (group[which] for group in groups[:3])
        at = fill(dims, row_ref[0], children.at[0], coupling[0], pivots[0], out_ref)
        for other in groups[3:]:
            held = dims[1]
            for child in range(2):
                for plane in range(other[which].shape[-1] // LANES):
                    out_ref[at : at + held, :] = other[which][0, child, :, plane * LANES : (plane + 1) * LANES]
                    at += held


def inner_kernel(*refs):
    count = (len(refs) - 1) // 2
    for in_ref, out_ref in zip(refs[1 : 1 + count], refs[1 + count :]):
        out_ref[...] = in_ref[0]


def assemble(dims, row, map_ref, in_ref, inners, hot_ref, half_ref, sum_ref, aug_ref, coup_ref):
    n, held, extra_rows, update_rows, pivot_rows = dims
    half = n // 2
    width = map_ref.shape[-1]
    span = half * held
    order = sum_ref.shape[0]
    size = aug_ref.shape[0]
    f32, bf16 = jnp.float32, jnp.bfloat16

    def hot(indices):
        place = lax.broadcasted_iota(jnp.int32, (order, indices.shape[-1]), 0)
        return jnp.where(place == indices, 1.0, 0.0).astype(bf16)

    last = (((1,), (1,)), ((), ()))

    def spread(values, table):
        high, low = split2(values)
        both = jnp.concatenate([high, low], axis=0)
        return lax.dot_general(both, table, last, preferred_element_type=f32).astype(bf16)

    lane = lax.broadcasted_iota(jnp.int32, (extra_rows, LANES), 1)
    lane8 = lax.broadcasted_iota(jnp.int32, (8, LANES), 1)
    pieces = held // extra_rows
    for child in range(2):
        indices = map_ref[0, child : child + 1, :]
        hot_ref[:, child * width : (child + 1) * width] = hot(indices)
        for source in range(n):
            place = source % half
            start = source // half * span
            turned = jnp.broadcast_to(indices[:, start : start + span], (8, span))
            if place:
                turned = pltpu.roll(turned, span - place * held, 1)
            values = in_ref[source, child * held : (child + 1) * held, :]
            table = turned[:1, :LANES]
            if (place < half // 2) == (child == 0):
                extra = in_ref[source, 2 * held : 2 * held + extra_rows, :]
                values = jnp.concatenate(
                    [
                        values,
                        jnp.concatenate(
                            [jnp.where(lane // held == piece, extra, 0.0) for piece in range(pieces)], axis=0
                        ),
                    ],
                    axis=1,
                )
                far = turned[:, LANES : 2 * LANES]
                tiled = far
                for piece in range(1, pieces):
                    tiled = jnp.where(lane8 // held == piece, pltpu.roll(far, piece * held, 1), tiled)
                table = jnp.concatenate([table, tiled[:1]], axis=1)
            moved = spread(values, hot(table))
            at = child * width + source * held
            half_ref[at : at + held, :] = moved[:held]
            half_ref[2 * width + at : 2 * width + at + held, :] = moved[held:]
        other = hot(jnp.where(row // half == 0, indices[:, span:], indices[:, :span]))
        for flip in range(half):
            moved = spread(inners(flip, child), other)
            at = pl.multiple_of(child * width + (row ^ flip) * held, held)
            half_ref[pl.ds(at, held), :] += moved[:held]
            half_ref[pl.ds(2 * width + at, held), :] += moved[held:]
    for block in range(order // LANES):
        rows = pl.ds(block * LANES, LANES)
        sum_ref[rows, :] = jnp.dot(
            hot_ref[rows, :], half_ref[: 2 * width, :], preferred_element_type=f32
        ) + jnp.dot(hot_ref[rows, :], half_ref[2 * width :, :], preferred_element_type=f32)

    at = 2 * held + extra_rows
    for source in range(n):
        coup_ref[source * update_rows : (source + 1) * update_rows, :] = in_ref[
            source, at : at + update_rows, :
        ]
        aug_ref[source * pivot_rows : (source + 1) * pivot_rows, :size] = in_ref[
            source, at + update_rows : at + update_rows + pivot_rows, :
        ]
    coup_ref[...] += sum_ref[size:, :size] + sum_ref[:size, size:].T
    aug_ref[:, :size] += sum_ref[:size, :size] + sum_ref[:size, :size].T
    square = (size, size)
    aug_ref[:, size:] = jnp.where(
        lax.broadcasted_iota(jnp.int32, square, 0) == lax.broadcasted_iota(jnp.int32, square, 1), 1.0, 0.0
    )


def eliminate(aug_ref):
    size = aug_ref.shape[0]
    lanes = lax.broadcasted_iota(jnp.int32, (1, size), 1)
    step = 32
    pivots = jnp.zeros((1, size), jnp.float32)
    for start in range(0, size, step):
        rest = size - start
        below = start + lax.broadcasted_iota(jnp.int32, (rest, 1), 0)

        def one(k, pivots, start=start, below=below):
            row = aug_ref[pl.ds(k, 1), :]
            whole = aug_ref[start:, :]
            chosen = lanes == k
            column = jnp.sum(jnp.where(chosen, whole[:, :size], 0.0), axis=1, keepdims=True)
            pivot = jnp.sum(jnp.where(chosen, row[:, :size], 0.0), axis=1, keepdims=True)
            multiplier = jnp.where(below > k, column / pivot, 0.0)
            aug_ref[start:, :] = whole - multiplier * row
            return jnp.where(chosen, pivot, pivots)

        pivots = lax.fori_loop(start, start + step, one, pivots)
    return pivots


def trailing(sum_ref, size, start):
    here = size + start
    return sum_ref[here : here + LANES, size:] + sum_ref[size:, here : here + LANES].T


LAST = (((1,), (1,)), ((), ()))


def update(out_ref, coup_ref, inverse, pivots, trailing_rows):
    size = inverse.shape[0]
    f32 = jnp.float32
    lhat = lax.dot_general(coup_ref[...], inverse, LAST, precision=highest, preferred_element_type=f32)
    out_ref[:, :size] = lhat
    coup_ref[...] = lhat / pivots
    for start in range(0, out_ref.shape[0], LANES):
        rows = pl.ds(start, LANES)
        correction = lax.dot_general(
            coup_ref[rows, :], out_ref[:, :size], LAST, precision=highest, preferred_element_type=f32
        )
        out_ref[rows, size:] = trailing_rows(start) - correction


def front_kernel(dims, row_ref, map_ref, *refs):
    n, held = dims[:2]
    out_ref, pivots_ref, hot_ref, half_ref, sum_ref, aug_ref, coup_ref, in_ref = refs[n:]
    rows = in_ref.shape[1]
    for flip in range(n):
        in_ref[row_ref[0] ^ flip] = refs[flip][:rows, :]

    def inners(flip, child):
        planes = (refs[flip].shape[0] - rows) // (2 * held)
        start = rows + child * planes * held
        return jnp.concatenate(
            [refs[flip][start + plane * held : start + (plane + 1) * held, :] for plane in range(planes)], axis=1
        )

    assemble(dims, row_ref[0], map_ref, in_ref, inners, hot_ref, half_ref, sum_ref, aug_ref, coup_ref)
    size = aug_ref.shape[0]
    pivots = eliminate(aug_ref)
    pivots_ref[...] = pivots
    update(out_ref, coup_ref, aug_ref[:, size:], pivots, functools.partial(trailing, sum_ref, size))


def factor_kernel(dims, row_ref, map_ref, in_ref, *refs):
    half = dims[0] // 2
    trail_ref, coup_ref, inverse_ref, pivots_ref, hot_ref, half_ref, sum_ref, aug_ref = refs[half:]
    inners = lambda flip, child: refs[flip][child]
    assemble(dims, row_ref[0], map_ref, in_ref, inners, hot_ref, half_ref, sum_ref, aug_ref, coup_ref)
    size = aug_ref.shape[0]
    pivots_ref[...] = eliminate(aug_ref)
    inverse_ref[...] = aug_ref[:, size:]
    for start in range(0, trail_ref.shape[0], LANES):
        trail_ref[pl.ds(start, LANES), :] = trailing(sum_ref, size, start)


def schur_kernel(row_ref, count_ref, trail_ref, coup_in_ref, inverse_ref, pivots_ref, *refs):
    out_refs = refs[:-2]
    full_ref, coup_ref = refs[-2:]
    coup_ref[...] = coup_in_ref[...]
    update(
        full_ref, coup_ref, inverse_ref[...], pivots_ref[...], lambda start: trail_ref[pl.ds(start, LANES), :]
    )
    update_rows, order = out_refs[0].shape
    size = inverse_ref.shape[0]
    shape = (8, order)
    first = lax.broadcasted_iota(jnp.int32, shape, 0)
    second = lax.broadcasted_iota(jnp.int32, shape, 1)
    for flip, out_ref in enumerate(out_refs):
        home = row_ref[0] ^ flip
        at = pl.multiple_of(home * update_rows, 8)
        out_ref[...] = full_ref[pl.ds(at, update_rows), :]
        chosen = (first == 1) & (second == size + at)
        out_ref[:8, :] = jnp.where(chosen, count_ref[0], full_ref[pl.ds(at, 8), :])


def finish_kernel(size, update_ref, back_ref, *refs):
    lhat_ref, schur_ref = refs[-2:]
    count = update_ref.shape[0]
    rows = pl.ds(pl.program_id(0) * count, count)
    lhat_ref[:, 0] = back_ref[rows, :, :size]
    schur_ref[:, 0] = update_ref[:, 0, :, size:] + back_ref[rows, :, size:]


def last_kernel(size, count, row_ref, update_ref, *refs):
    back_refs, seen_ref = refs[:count], refs[count]
    lhat_ref, schur_ref, total_ref = refs[-3:]
    step = pl.program_id(0)
    update_rows, order = back_refs[0].shape
    shape = (8, order - size)
    first = lax.broadcasted_iota(jnp.int32, shape, 0)
    second = lax.broadcasted_iota(jnp.int32, shape, 1)
    at = row_ref[0] * update_rows

    @pl.when(step == 0)
    def _():
        total_ref[...] = seen_ref[...]

    for which in range(count):

        @pl.when(step == which)
        def _(which=which):
            back = back_refs[which]
            lhat_ref[0] = back[:, :size]
            schur_ref[0] = update_ref[0, :, size:] + back[:, size:]
            head = back[:8, size:]
            marked = (first == 1) & (second == at)
            twin = jnp.sum(jnp.where((first == 0) & (second == at + 1), head, 0.0))
            total_ref[...] += jnp.sum(jnp.where(marked, head, 0.0))
            schur_ref[0, :8, :] = update_ref[0, :8, size:] + jnp.where(marked, twin, head)


def local_body(front_pivot, front_update, child_blocks, child_map):
    f32 = jnp.float32
    n = lax.axis_size("row")
    half = n // 2
    my_row = lax.axis_index("row")
    fronts, pivot_rows, size = front_pivot.shape
    update_rows, order = front_update.shape[1:]
    held, width = child_blocks.shape[2:]
    per = fronts // n
    span = half * held
    extra_rows = held * held // LANES
    rows = 2 * held + extra_rows + update_rows + pivot_rows
    row_number = my_row.astype(jnp.int32).reshape(1)
    dims = (n, held, extra_rows)
    group = n // 2
    vmem = pl.BlockSpec(memory_space=pltpu.VMEM)
    whole = pl.BlockSpec(memory_space=pl.ANY)
    updates = front_update.reshape(n, per, update_rows, order)
    flat = jax.ShapeDtypeStruct

    def pack(turn):
        return pl.pallas_call(
            functools.partial(pack_kernel, dims),
            grid_spec=pltpu.PrefetchScalarGridSpec(
                num_scalar_prefetch=1,
                grid=(n // group,),
                in_specs=[
                    pl.BlockSpec((group, 1, 2, held, span), lambda g, r: (g, turn, 0, 0, r[0] // half)),
                    pl.BlockSpec((group, 1, update_rows, size), lambda g, r: (g, turn, 0, 0)),
                    pl.BlockSpec((group, 1, pivot_rows, size), lambda g, r: (g, turn, 0, 0)),
                ],
                out_specs=pl.BlockSpec((group, rows, LANES), lambda g, r: (g, 0, 0)),
            ),
            out_shape=flat((n, rows, LANES), f32),
            name="pack",
        )(
            row_number,
            child_blocks.reshape(n, per, 2, held, width),
            updates,
            front_pivot.reshape(n, per, pivot_rows, size),
        )

    def parts_for(turn, flips):
        near = flips[0] < half

        def front(r, flip):
            return (r[0] ^ flip) * per + turn

        specs = [
            pl.BlockSpec((1, 2, held, span), lambda g, r, f=f: (front(r, f), 0, 0, r[0] // half)) for f in flips
        ]
        specs += [pl.BlockSpec((1, update_rows, size), lambda g, r, f=f: (front(r, f), 0, 0)) for f in flips]
        specs += [pl.BlockSpec((1, pivot_rows, size), lambda g, r, f=f: (front(r, f), 0, 0)) for f in flips]
        if near:
            specs += [
                pl.BlockSpec((1, 2, held, span), lambda g, r, f=f: (front(r, f), 0, 0, 1 - r[0] // half))
                for f in flips
            ]
        count = len(flips)
        operands = [child_blocks] * count + [front_update] * count + [front_pivot] * count
        operands += [child_blocks] * count if near else []
        return pl.pallas_call(
            functools.partial(part_kernel, dims, count),
            grid_spec=pltpu.PrefetchScalarGridSpec(
                num_scalar_prefetch=1, grid=(1,), in_specs=specs, out_specs=[vmem] * count
            ),
            out_shape=[flat((rows + (2 * held * span // LANES if near else 0), LANES), f32)] * count,
            name="parts",
        )(row_number, *operands)

    def inner(turn):
        def spec(flip):
            return pl.BlockSpec(
                (1, 2, held, span), lambda g, r: ((r[0] ^ flip) * per + turn, 0, 0, 1 - r[0] // half)
            )

        return pl.pallas_call(
            inner_kernel,
            grid_spec=pltpu.PrefetchScalarGridSpec(
                num_scalar_prefetch=1,
                grid=(1,),
                in_specs=[spec(flip) for flip in range(half)],
                out_specs=[vmem] * half,
            ),
            out_shape=[flat((2, held, span), f32)] * half,
            name="inner",
        )(row_number, *[child_blocks] * half)

    def from_arrived(kernel, arrays, turn, outs, scratch):
        return pl.pallas_call(
            functools.partial(kernel, dims + (update_rows, pivot_rows)),
            grid_spec=pltpu.PrefetchScalarGridSpec(
                num_scalar_prefetch=1,
                grid=(1,),
                in_specs=[pl.BlockSpec((1, 2, width), lambda g, r: (r[0] * per + turn, 0, 0))]
                + [vmem] * len(arrays),
                out_specs=(vmem,) * len(outs),
                scratch_shapes=[
                    pltpu.VMEM((order, 2 * width), jnp.bfloat16),
                    pltpu.VMEM((4 * width, order), jnp.bfloat16),
                    pltpu.VMEM((order, order), f32),
                    pltpu.VMEM((size, 2 * size), f32),
                ]
                + scratch,
            ),
            out_shape=tuple(flat(shape, f32) for shape in outs),
            name="front",
        )(row_number, child_map, *arrays)

    def whole_front(arrays, turn):
        outs = [(order - size, order), (1, size)]
        scratch = [pltpu.VMEM((order - size, size), f32), pltpu.VMEM((n, rows, LANES), f32)]
        return from_arrived(front_kernel, arrays, turn, outs, scratch)

    def factored(arrays, turn):
        outs = [(order - size, order - size), (order - size, size), (size, size), (1, size)]
        return from_arrived(factor_kernel, arrays, turn, outs, [])

    def schur_rows(count, parts):
        smem = pl.BlockSpec(memory_space=pltpu.SMEM)
        return pl.pallas_call(
            schur_kernel,
            in_specs=[smem, smem] + [vmem] * 4,
            out_specs=[vmem] * n,
            out_shape=[flat((update_rows, order), f32)] * n,
            scratch_shapes=[pltpu.VMEM((order - size, order), f32), pltpu.VMEM((order - size, size), f32)],
            name="schur",
        )(row_number, count.reshape(1), *parts)

    def finish(back, turn, before):
        aliases = {2: 0, 3: 1} if before else {}
        group = 2
        place = lambda g: (g, turn, 0, 0)
        return pl.pallas_call(
            functools.partial(finish_kernel, size),
            grid=(n // group,),
            in_specs=[pl.BlockSpec((group, 1, update_rows, order), place), vmem] + [whole] * len(before),
            out_specs=(
                pl.BlockSpec((group, 1, update_rows, size), place),
                pl.BlockSpec((group, 1, update_rows, order - size), place),
            ),
            out_shape=(
                flat((n, per, update_rows, size), f32),
                flat((n, per, update_rows, order - size), f32),
            ),
            input_output_aliases=aliases,
            name="finish",
        )(updates, back, *before)

    def last(backs, flips, turn, before, seen):
        count = len(backs)
        place = lambda g, r: ((r[0] ^ (flips[0] + g)) * per + turn, 0, 0)
        before = [part.reshape(fronts, update_rows, -1) for part in before]
        aliases = {3 + count: 0, 4 + count: 1} if before else {}
        return pl.pallas_call(
            functools.partial(last_kernel, size, count),
            grid_spec=pltpu.PrefetchScalarGridSpec(
                num_scalar_prefetch=1,
                grid=(count,),
                in_specs=[pl.BlockSpec((1, update_rows, order), place)]
                + [vmem] * (count + 1)
                + [whole] * len(before),
                out_specs=(
                    pl.BlockSpec((1, update_rows, size), place),
                    pl.BlockSpec((1, update_rows, order - size), place),
                    pl.BlockSpec((1, size), lambda g, r: (0, 0)),
                ),
            ),
            out_shape=(
                flat((fronts, update_rows, size), f32),
                flat((fronts, update_rows, order - size), f32),
                flat((1, size), f32),
            ),
            input_output_aliases=aliases,
            name="last",
        )(row_number, front_update, *backs, seen, *before)

    exchange = functools.partial(lax.all_to_all, axis_name="row", split_axis=0, concat_axis=0, tiled=True)

    def send(part, flip):
        return lax.ppermute(part, "row", [(i, i ^ flip) for i in range(n)])

    arrays = []
    for turn in range(per - 1):
        far = parts_for(turn, range(half, n))
        far = [send(part, half + flip) for flip, part in enumerate(far)]
        near = parts_for(turn, range(half))
        near = [near[0]] + [send(near[flip], flip) for flip in range(1, half)]
        arrays.append(near + far)
    turn = per - 1
    packed = pack(turn)
    arrived = exchange(packed)
    parts = inner(turn)
    arrays.append([arrived, parts[0]] + [send(parts[flip], flip) for flip in range(1, half)])
    total = jnp.zeros((), f32)
    backs = []
    for turn in range(per - 1):
        rows_out, pivots = whole_front(arrays[turn], turn)
        total = total + jnp.sum(jnp.where(pivots < 0.0, 1.0, 0.0))
        backs.append(exchange(rows_out.reshape(n, update_rows, order)))
    turn = per - 1
    parts = factored(arrays[turn], turn)
    total = lax.psum(total + jnp.sum(jnp.where(parts[3] < 0.0, 1.0, 0.0)), "col")
    homes = schur_rows(total, parts)
    homes = [homes[0]] + [send(homes[flip], flip) for flip in range(1, n)]
    done = ()
    for turn in range(per - 1):
        done = finish(backs[turn], turn, done)
    seen = jnp.zeros((1, size), f32)
    for begin, end in [(0, half)] + [(flip, flip + 1) for flip in range(half, n)]:
        flips = range(begin, end)
        lhat, schur, seen = last([homes[flip] for flip in flips], flips, per - 1, done, seen)
        done = (lhat, schur)
    negative_share = seen[0, 0] / (fronts * lax.axis_size("col") * size)
    return (lhat, schur, negative_share)


def solution(mesh):
    in_specs = (
        P("col", "row", None),
        P("col", "row", None),
        P("col", None, "row", None),
        P("col", None, None),
    )
    out_specs = (P("col", "row", None), P("col", "row", None), P())
    return jax.shard_map(local_body, mesh=mesh, in_specs=in_specs, out_specs=out_specs, check_vma=False)
```

```python
import functools

import jax
import jax.numpy as jnp
from jax import lax
from jax.experimental import pallas as pl
from jax.experimental.pallas import tpu as pltpu
from jax.sharding import PartitionSpec as P


LANES = 128
highest = lax.Precision.HIGHEST


def split2(x):
    high = x.astype(jnp.bfloat16)
    low = (x - high.astype(jnp.float32)).astype(jnp.bfloat16)
    return high, low


def fill(dims, row, children, coupling, pivots, out_ref):
    n, held, extra_rows = dims
    half = n // 2
    span = half * held
    place = lax.rem(row, half)
    lane = lax.broadcasted_iota(jnp.int32, (held, LANES), 1)
    lane_extra = lax.broadcasted_iota(jnp.int32, (extra_rows, LANES), 1)
    extras = []
    at = 0
    for child in range(2):
        rolled = pltpu.roll(children[child], lax.rem(span - place * held, span), 1)
        near = rolled[:, :LANES]
        out_ref[at : at + held, :] = jnp.where(lane < held, 0.5 * near, near)
        at += held
        extras.append(rolled[:, LANES:])
    extra = jnp.where(place < half // 2, extras[0], extras[1])
    packed = extra[:extra_rows]
    for piece in range(1, held // extra_rows):
        rows = pltpu.roll(extra[piece * extra_rows : (piece + 1) * extra_rows], piece * held, 1)
        packed = jnp.where(lane_extra // held == piece, rows, packed)
    for part in (packed, coupling, pivots):
        out_ref[at : at + part.shape[0], :] = part
        at += part.shape[0]
    return at


def pack_kernel(dims, row_ref, child_ref, update_ref, pivot_ref, out_ref):
    for front in range(child_ref.shape[0]):
        fill(
            dims, row_ref[0], child_ref.at[front, 0], update_ref[front, 0], pivot_ref[front, 0], out_ref.at[front]
        )


def part_kernel(dims, count, row_ref, *refs):
    inputs, outs = refs[:-count], refs[-count:]
    groups = [inputs[at : at + count] for at in range(0, len(inputs), count)]
    for which, out_ref in enumerate(outs):
        children, coupling, pivots = (group[which] for group in groups[:3])
        at = fill(dims, row_ref[0], children.at[0], coupling[0], pivots[0], out_ref)
        for other in groups[3:]:
            held = dims[1]
            for child in range(2):
                for plane in range(other[which].shape[-1] // LANES):
                    out_ref[at : at + held, :] = other[which][0, child, :, plane * LANES : (plane + 1) * LANES]
                    at += held


def inner_kernel(*refs):
    count = (len(refs) - 1) // 2
    for in_ref, out_ref in zip(refs[1 : 1 + count], refs[1 + count :]):
        out_ref[...] = in_ref[0]


def assemble(dims, row, map_ref, in_ref, inners, hot_ref, half_ref, sum_ref, aug_ref, coup_ref):
    n, held, extra_rows, update_rows, pivot_rows = dims
    half = n // 2
    width = map_ref.shape[-1]
    span = half * held
    order = sum_ref.shape[0]
    size = aug_ref.shape[0]
    f32, bf16 = jnp.float32, jnp.bfloat16

    def hot(indices):
        place = lax.broadcasted_iota(jnp.int32, (order, indices.shape[-1]), 0)
        return jnp.where(place == indices, 1.0, 0.0).astype(bf16)

    last = (((1,), (1,)), ((), ()))

    def spread(values, table):
        high, low = split2(values)
        both = jnp.concatenate([high, low], axis=0)
        return lax.dot_general(both, table, last, preferred_element_type=f32).astype(bf16)

    lane = lax.broadcasted_iota(jnp.int32, (extra_rows, LANES), 1)
    lane8 = lax.broadcasted_iota(jnp.int32, (8, LANES), 1)
    pieces = held // extra_rows
    for child in range(2):
        indices = map_ref[0, child : child + 1, :]
        hot_ref[:, child * width : (child + 1) * width] = hot(indices)
        for source in range(n):
            place = source % half
            start = source // half * span
            turned = jnp.broadcast_to(indices[:, start : start + span], (8, span))
            if place:
                turned = pltpu.roll(turned, span - place * held, 1)
            values = in_ref[source, child * held : (child + 1) * held, :]
            table = turned[:1, :LANES]
            if (place < half // 2) == (child == 0):
                extra = in_ref[source, 2 * held : 2 * held + extra_rows, :]
                values = jnp.concatenate(
                    [
                        values,
                        jnp.concatenate(
                            [jnp.where(lane // held == piece, extra, 0.0) for piece in range(pieces)], axis=0
                        ),
                    ],
                    axis=1,
                )
                far = turned[:, LANES : 2 * LANES]
                tiled = far
                for piece in range(1, pieces):
                    tiled = jnp.where(lane8 // held == piece, pltpu.roll(far, piece * held, 1), tiled)
                table = jnp.concatenate([table, tiled[:1]], axis=1)
            moved = spread(values, hot(table))
            at = child * width + source * held
            half_ref[at : at + held, :] = moved[:held]
            half_ref[2 * width + at : 2 * width + at + held, :] = moved[held:]
        other = hot(jnp.where(row // half == 0, indices[:, span:], indices[:, :span]))
        for flip in range(half):
            moved = spread(inners(flip, child), other)
            at = pl.multiple_of(child * width + (row ^ flip) * held, held)
            half_ref[pl.ds(at, held), :] += moved[:held]
            half_ref[pl.ds(2 * width + at, held), :] += moved[held:]
    for block in range(order // LANES):
        rows = pl.ds(block * LANES, LANES)
        sum_ref[rows, :] = jnp.dot(
            hot_ref[rows, :], half_ref[: 2 * width, :], preferred_element_type=f32
        ) + jnp.dot(hot_ref[rows, :], half_ref[2 * width :, :], preferred_element_type=f32)

    at = 2 * held + extra_rows
    for source in range(n):
        coup_ref[source * update_rows : (source + 1) * update_rows, :] = in_ref[
            source, at : at + update_rows, :
        ]
        aug_ref[source * pivot_rows : (source + 1) * pivot_rows, :size] = in_ref[
            source, at + update_rows : at + update_rows + pivot_rows, :
        ]
    coup_ref[...] += sum_ref[size:, :size] + sum_ref[:size, size:].T
    aug_ref[:, :size] += sum_ref[:size, :size] + sum_ref[:size, :size].T
    square = (size, size)
    aug_ref[:, size:] = jnp.where(
        lax.broadcasted_iota(jnp.int32, square, 0) == lax.broadcasted_iota(jnp.int32, square, 1), 1.0, 0.0
    )


def eliminate(aug_ref):
    size = aug_ref.shape[0]
    panel = 16
    shape = (panel, size)
    sub = lax.broadcasted_iota(jnp.int32, shape, 0)
    lane = lax.broadcasted_iota(jnp.int32, shape, 1)

    def one(block, pivots):
        base = pl.multiple_of(block * panel, panel)
        left = aug_ref[pl.ds(base, panel), :size]
        right = aug_ref[pl.ds(base, panel), size:]
        turned = pltpu.roll(left, lax.rem(size - base, size), 1)
        columns = [jnp.broadcast_to(turned[:, j : j + 1], shape) for j in range(panel)]
        scale = jnp.zeros(shape, jnp.float32)
        for j in range(panel):
            pivot = columns[j][j : j + 1, :]
            inverse = 1.0 / pivot
            multiplier = jnp.where(sub > j, columns[j] * inverse, 0.0)
            for k in range(j + 1, panel):
                columns[k] = columns[k] - multiplier * columns[k][j : j + 1, :]
            left = left - multiplier * left[j : j + 1, :]
            right = right - multiplier * right[j : j + 1, :]
            scale = jnp.where(sub == j, inverse, scale)
            pivots = jnp.where(lane[:1] == base + j, pivot, pivots)
        aug_ref[pl.ds(base, panel), :size] = left
        aug_ref[pl.ds(base, panel), size:] = right
        lower = jnp.where(lane >= base + panel, left * scale, 0.0)
        both = jnp.concatenate([left, right], axis=1)
        aug_ref[...] -= lax.dot_general(
            lower, both, (((0,), (0,)), ((), ())), precision=highest, preferred_element_type=jnp.float32
        )
        return pivots

    return lax.fori_loop(0, size // panel, one, jnp.zeros((1, size), jnp.float32))


def trailing(sum_ref, size, start):
    here = size + start
    return sum_ref[here : here + LANES, size:] + sum_ref[size:, here : here + LANES].T


LAST = (((1,), (1,)), ((), ()))


def update(out_ref, coup_ref, inverse, pivots, trailing_rows):
    size = inverse.shape[0]
    f32 = jnp.float32
    lhat = lax.dot_general(coup_ref[...], inverse, LAST, precision=highest, preferred_element_type=f32)
    out_ref[:, :size] = lhat
    coup_ref[...] = lhat / pivots
    for start in range(0, out_ref.shape[0], LANES):
        rows = pl.ds(start, LANES)
        correction = lax.dot_general(
            coup_ref[rows, :], out_ref[:, :size], LAST, precision=highest, preferred_element_type=f32
        )
        out_ref[rows, size:] = trailing_rows(start) - correction


def front_kernel(dims, row_ref, map_ref, *refs):
    n, held = dims[:2]
    out_ref, pivots_ref, hot_ref, half_ref, sum_ref, aug_ref, coup_ref, in_ref = refs[n:]
    rows = in_ref.shape[1]
    for flip in range(n):
        in_ref[row_ref[0] ^ flip] = refs[flip][:rows, :]

    def inners(flip, child):
        planes = (refs[flip].shape[0] - rows) // (2 * held)
        start = rows + child * planes * held
        return jnp.concatenate(
            [refs[flip][start + plane * held : start + (plane + 1) * held, :] for plane in range(planes)], axis=1
        )

    assemble(dims, row_ref[0], map_ref, in_ref, inners, hot_ref, half_ref, sum_ref, aug_ref, coup_ref)
    size = aug_ref.shape[0]
    pivots = eliminate(aug_ref)
    pivots_ref[...] = pivots
    update(out_ref, coup_ref, aug_ref[:, size:], pivots, functools.partial(trailing, sum_ref, size))


def factor_kernel(dims, row_ref, map_ref, in_ref, *refs):
    half = dims[0] // 2
    trail_ref, coup_ref, inverse_ref, pivots_ref, hot_ref, half_ref, sum_ref, aug_ref = refs[half:]
    inners = lambda flip, child: refs[flip][child]
    assemble(dims, row_ref[0], map_ref, in_ref, inners, hot_ref, half_ref, sum_ref, aug_ref, coup_ref)
    size = aug_ref.shape[0]
    pivots_ref[...] = eliminate(aug_ref)
    inverse_ref[...] = aug_ref[:, size:]
    for start in range(0, trail_ref.shape[0], LANES):
        trail_ref[pl.ds(start, LANES), :] = trailing(sum_ref, size, start)


def schur_kernel(row_ref, count_ref, trail_ref, coup_in_ref, inverse_ref, pivots_ref, *refs):
    out_refs = refs[:-2]
    full_ref, coup_ref = refs[-2:]
    coup_ref[...] = coup_in_ref[...]
    update(
        full_ref, coup_ref, inverse_ref[...], pivots_ref[...], lambda start: trail_ref[pl.ds(start, LANES), :]
    )
    update_rows, order = out_refs[0].shape
    size = inverse_ref.shape[0]
    shape = (8, order)
    first = lax.broadcasted_iota(jnp.int32, shape, 0)
    second = lax.broadcasted_iota(jnp.int32, shape, 1)
    for flip, out_ref in enumerate(out_refs):
        home = row_ref[0] ^ flip
        at = pl.multiple_of(home * update_rows, 8)
        out_ref[...] = full_ref[pl.ds(at, update_rows), :]
        chosen = (first == 1) & (second == size + at)
        out_ref[:8, :] = jnp.where(chosen, count_ref[0], full_ref[pl.ds(at, 8), :])


def finish_kernel(size, update_ref, back_ref, *refs):
    lhat_ref, schur_ref = refs[-2:]
    count = update_ref.shape[0]
    rows = pl.ds(pl.program_id(0) * count, count)
    lhat_ref[:, 0] = back_ref[rows, :, :size]
    schur_ref[:, 0] = update_ref[:, 0, :, size:] + back_ref[rows, :, size:]


def last_kernel(size, count, row_ref, update_ref, *refs):
    back_refs, seen_ref = refs[:count], refs[count]
    lhat_ref, schur_ref, total_ref = refs[-3:]
    step = pl.program_id(0)
    update_rows, order = back_refs[0].shape
    shape = (8, order - size)
    first = lax.broadcasted_iota(jnp.int32, shape, 0)
    second = lax.broadcasted_iota(jnp.int32, shape, 1)
    at = row_ref[0] * update_rows

    @pl.when(step == 0)
    def _():
        total_ref[...] = seen_ref[...]

    for which in range(count):

        @pl.when(step == which)
        def _(which=which):
            back = back_refs[which]
            lhat_ref[0] = back[:, :size]
            schur_ref[0] = update_ref[0, :, size:] + back[:, size:]
            head = back[:8, size:]
            marked = (first == 1) & (second == at)
            twin = jnp.sum(jnp.where((first == 0) & (second == at + 1), head, 0.0))
            total_ref[...] += jnp.sum(jnp.where(marked, head, 0.0))
            schur_ref[0, :8, :] = update_ref[0, :8, size:] + jnp.where(marked, twin, head)


def local_body(front_pivot, front_update, child_blocks, child_map):
    f32 = jnp.float32
    n = lax.axis_size("row")
    half = n // 2
    my_row = lax.axis_index("row")
    fronts, pivot_rows, size = front_pivot.shape
    update_rows, order = front_update.shape[1:]
    held, width = child_blocks.shape[2:]
    per = fronts // n
    span = half * held
    extra_rows = held * held // LANES
    rows = 2 * held + extra_rows + update_rows + pivot_rows
    row_number = my_row.astype(jnp.int32).reshape(1)
    dims = (n, held, extra_rows)
    group = n // 2
    vmem = pl.BlockSpec(memory_space=pltpu.VMEM)
    whole = pl.BlockSpec(memory_space=pl.ANY)
    updates = front_update.reshape(n, per, update_rows, order)
    flat = jax.ShapeDtypeStruct

    def pack(turn):
        return pl.pallas_call(
            functools.partial(pack_kernel, dims),
            grid_spec=pltpu.PrefetchScalarGridSpec(
                num_scalar_prefetch=1,
                grid=(n // group,),
                in_specs=[
                    pl.BlockSpec((group, 1, 2, held, span), lambda g, r: (g, turn, 0, 0, r[0] // half)),
                    pl.BlockSpec((group, 1, update_rows, size), lambda g, r: (g, turn, 0, 0)),
                    pl.BlockSpec((group, 1, pivot_rows, size), lambda g, r: (g, turn, 0, 0)),
                ],
                out_specs=pl.BlockSpec((group, rows, LANES), lambda g, r: (g, 0, 0)),
            ),
            out_shape=flat((n, rows, LANES), f32),
            name="pack",
        )(
            row_number,
            child_blocks.reshape(n, per, 2, held, width),
            updates,
            front_pivot.reshape(n, per, pivot_rows, size),
        )

    def parts_for(turn, flips):
        near = flips[0] < half

        def front(r, flip):
            return (r[0] ^ flip) * per + turn

        specs = [
            pl.BlockSpec((1, 2, held, span), lambda g, r, f=f: (front(r, f), 0, 0, r[0] // half)) for f in flips
        ]
        specs += [pl.BlockSpec((1, update_rows, size), lambda g, r, f=f: (front(r, f), 0, 0)) for f in flips]
        specs += [pl.BlockSpec((1, pivot_rows, size), lambda g, r, f=f: (front(r, f), 0, 0)) for f in flips]
        if near:
            specs += [
                pl.BlockSpec((1, 2, held, span), lambda g, r, f=f: (front(r, f), 0, 0, 1 - r[0] // half))
                for f in flips
            ]
        count = len(flips)
        operands = [child_blocks] * count + [front_update] * count + [front_pivot] * count
        operands += [child_blocks] * count if near else []
        return pl.pallas_call(
            functools.partial(part_kernel, dims, count),
            grid_spec=pltpu.PrefetchScalarGridSpec(
                num_scalar_prefetch=1, grid=(1,), in_specs=specs, out_specs=[vmem] * count
            ),
            out_shape=[flat((rows + (2 * held * span // LANES if near else 0), LANES), f32)] * count,
            name="parts",
        )(row_number, *operands)

    def inner(turn):
        def spec(flip):
            return pl.BlockSpec(
                (1, 2, held, span), lambda g, r: ((r[0] ^ flip) * per + turn, 0, 0, 1 - r[0] // half)
            )

        return pl.pallas_call(
            inner_kernel,
            grid_spec=pltpu.PrefetchScalarGridSpec(
                num_scalar_prefetch=1,
                grid=(1,),
                in_specs=[spec(flip) for flip in range(half)],
                out_specs=[vmem] * half,
            ),
            out_shape=[flat((2, held, span), f32)] * half,
            name="inner",
        )(row_number, *[child_blocks] * half)

    def from_arrived(kernel, arrays, turn, outs, scratch):
        return pl.pallas_call(
            functools.partial(kernel, dims + (update_rows, pivot_rows)),
            grid_spec=pltpu.PrefetchScalarGridSpec(
                num_scalar_prefetch=1,
                grid=(1,),
                in_specs=[pl.BlockSpec((1, 2, width), lambda g, r: (r[0] * per + turn, 0, 0))]
                + [vmem] * len(arrays),
                out_specs=(vmem,) * len(outs),
                scratch_shapes=[
                    pltpu.VMEM((order, 2 * width), jnp.bfloat16),
                    pltpu.VMEM((4 * width, order), jnp.bfloat16),
                    pltpu.VMEM((order, order), f32),
                    pltpu.VMEM((size, 2 * size), f32),
                ]
                + scratch,
            ),
            out_shape=tuple(flat(shape, f32) for shape in outs),
            name="front",
        )(row_number, child_map, *arrays)

    def whole_front(arrays, turn):
        outs = [(order - size, order), (1, size)]
        scratch = [pltpu.VMEM((order - size, size), f32), pltpu.VMEM((n, rows, LANES), f32)]
        return from_arrived(front_kernel, arrays, turn, outs, scratch)

    def factored(arrays, turn):
        outs = [(order - size, order - size), (order - size, size), (size, size), (1, size)]
        return from_arrived(factor_kernel, arrays, turn, outs, [])

    def schur_rows(count, parts):
        smem = pl.BlockSpec(memory_space=pltpu.SMEM)
        return pl.pallas_call(
            schur_kernel,
            in_specs=[smem, smem] + [vmem] * 4,
            out_specs=[vmem] * n,
            out_shape=[flat((update_rows, order), f32)] * n,
            scratch_shapes=[pltpu.VMEM((order - size, order), f32), pltpu.VMEM((order - size, size), f32)],
            name="schur",
        )(row_number, count.reshape(1), *parts)

    def finish(back, turn, before):
        aliases = {2: 0, 3: 1} if before else {}
        group = 2
        place = lambda g: (g, turn, 0, 0)
        return pl.pallas_call(
            functools.partial(finish_kernel, size),
            grid=(n // group,),
            in_specs=[pl.BlockSpec((group, 1, update_rows, order), place), vmem] + [whole] * len(before),
            out_specs=(
                pl.BlockSpec((group, 1, update_rows, size), place),
                pl.BlockSpec((group, 1, update_rows, order - size), place),
            ),
            out_shape=(
                flat((n, per, update_rows, size), f32),
                flat((n, per, update_rows, order - size), f32),
            ),
            input_output_aliases=aliases,
            name="finish",
        )(updates, back, *before)

    def last(backs, flips, turn, before, seen):
        count = len(backs)
        place = lambda g, r: ((r[0] ^ (flips[0] + g)) * per + turn, 0, 0)
        before = [part.reshape(fronts, update_rows, -1) for part in before]
        aliases = {3 + count: 0, 4 + count: 1} if before else {}
        return pl.pallas_call(
            functools.partial(last_kernel, size, count),
            grid_spec=pltpu.PrefetchScalarGridSpec(
                num_scalar_prefetch=1,
                grid=(count,),
                in_specs=[pl.BlockSpec((1, update_rows, order), place)]
                + [vmem] * (count + 1)
                + [whole] * len(before),
                out_specs=(
                    pl.BlockSpec((1, update_rows, size), place),
                    pl.BlockSpec((1, update_rows, order - size), place),
                    pl.BlockSpec((1, size), lambda g, r: (0, 0)),
                ),
            ),
            out_shape=(
                flat((fronts, update_rows, size), f32),
                flat((fronts, update_rows, order - size), f32),
                flat((1, size), f32),
            ),
            input_output_aliases=aliases,
            name="last",
        )(row_number, front_update, *backs, seen, *before)

    exchange = functools.partial(lax.all_to_all, axis_name="row", split_axis=0, concat_axis=0, tiled=True)

    def send(part, flip):
        return lax.ppermute(part, "row", [(i, i ^ flip) for i in range(n)])

    arrays = []
    for turn in range(per - 1):
        far = parts_for(turn, range(half, n))
        sent = [send(part, half + flip) for flip, part in enumerate(far[:-1])]
        far = sent + [send(far[-1], n - 1)]
        near = parts_for(turn, range(half))
        near = [near[0]] + [send(near[flip], flip) for flip in range(1, half)]
        arrays.append(near + far)
    turn = per - 1
    packed = pack(turn)
    arrived = exchange(packed)
    parts = inner(turn)
    arrays.append([arrived, parts[0]] + [send(parts[flip], flip) for flip in range(1, half)])
    total = jnp.zeros((), f32)
    backs = []
    for turn in range(per - 1):
        rows_out, pivots = whole_front(arrays[turn], turn)
        total = total + jnp.sum(jnp.where(pivots < 0.0, 1.0, 0.0))
        backs.append(exchange(rows_out.reshape(n, update_rows, order)))
    turn = per - 1
    parts = factored(arrays[turn], turn)
    total = lax.psum(total + jnp.sum(jnp.where(parts[3] < 0.0, 1.0, 0.0)), "col")
    homes = schur_rows(total, parts)
    homes = [homes[0]] + [send(homes[flip], flip) for flip in range(1, n)]
    done = ()
    for turn in range(per - 1):
        done = finish(backs[turn], turn, done)
    seen = jnp.zeros((1, size), f32)
    for begin, end in [(0, half)] + [(flip, flip + 1) for flip in range(half, n)]:
        flips = range(begin, end)
        lhat, schur, seen = last([homes[flip] for flip in flips], flips, per - 1, done, seen)
        done = (lhat, schur)
    negative_share = seen[0, 0] / (fronts * lax.axis_size("col") * size)
    return (lhat, schur, negative_share)


def solution(mesh):
    in_specs = (
        P("col", "row", None),
        P("col", "row", None),
        P("col", None, "row", None),
        P("col", None, None),
    )
    out_specs = (P("col", "row", None), P("col", "row", None), P())
    return jax.shard_map(local_body, mesh=mesh, in_specs=in_specs, out_specs=out_specs, check_vma=False)
```

```python
import functools

import jax
import jax.numpy as jnp
from jax import lax
from jax.experimental import pallas as pl
from jax.experimental.pallas import tpu as pltpu
from jax.sharding import PartitionSpec as P


LANES = 128
highest = lax.Precision.HIGHEST


def split2(x):
    high = x.astype(jnp.bfloat16)
    low = (x - high.astype(jnp.float32)).astype(jnp.bfloat16)
    return high, low


def fill(dims, row, children, coupling, pivots, out_ref):
    n, held, extra_rows = dims
    half = n // 2
    span = half * held
    place = lax.rem(row, half)
    lane = lax.broadcasted_iota(jnp.int32, (held, LANES), 1)
    lane_extra = lax.broadcasted_iota(jnp.int32, (extra_rows, LANES), 1)
    extras = []
    at = 0
    for child in range(2):
        rolled = pltpu.roll(children[child], lax.rem(span - place * held, span), 1)
        near = rolled[:, :LANES]
        out_ref[at : at + held, :] = jnp.where(lane < held, 0.5 * near, near)
        at += held
        extras.append(rolled[:, LANES:])
    extra = jnp.where(place < half // 2, extras[0], extras[1])
    packed = extra[:extra_rows]
    for piece in range(1, held // extra_rows):
        rows = pltpu.roll(extra[piece * extra_rows : (piece + 1) * extra_rows], piece * held, 1)
        packed = jnp.where(lane_extra // held == piece, rows, packed)
    for part in (packed, coupling, pivots):
        out_ref[at : at + part.shape[0], :] = part
        at += part.shape[0]
    return at


def pack_kernel(dims, row_ref, child_ref, update_ref, pivot_ref, out_ref):
    for front in range(child_ref.shape[0]):
        fill(
            dims, row_ref[0], child_ref.at[front, 0], update_ref[front, 0], pivot_ref[front, 0], out_ref.at[front]
        )


def part_kernel(dims, count, row_ref, *refs):
    inputs, outs = refs[:-count], refs[-count:]
    groups = [inputs[at : at + count] for at in range(0, len(inputs), count)]
    for which, out_ref in enumerate(outs):
        children, coupling, pivots = (group[which] for group in groups[:3])
        at = fill(dims, row_ref[0], children.at[0], coupling[0], pivots[0], out_ref)
        for other in groups[3:]:
            held = dims[1]
            for child in range(2):
                for plane in range(other[which].shape[-1] // LANES):
                    out_ref[at : at + held, :] = other[which][0, child, :, plane * LANES : (plane + 1) * LANES]
                    at += held


def inner_kernel(*refs):
    count = (len(refs) - 1) // 2
    for in_ref, out_ref in zip(refs[1 : 1 + count], refs[1 + count :]):
        out_ref[...] = in_ref[0]


def assemble(dims, row, map_ref, in_ref, inners, hot_ref, half_ref, sum_ref, aug_ref, coup_ref):
    n, held, extra_rows, update_rows, pivot_rows = dims
    half = n // 2
    width = map_ref.shape[-1]
    span = half * held
    order = sum_ref.shape[0]
    size = aug_ref.shape[0]
    f32, bf16 = jnp.float32, jnp.bfloat16

    def hot(indices):
        place = lax.broadcasted_iota(jnp.int32, (order, indices.shape[-1]), 0)
        return jnp.where(place == indices, 1.0, 0.0).astype(bf16)

    last = (((1,), (1,)), ((), ()))

    def spread(values, table):
        high, low = split2(values)
        both = jnp.concatenate([high, low], axis=0)
        return lax.dot_general(both, table, last, preferred_element_type=f32).astype(bf16)

    lane = lax.broadcasted_iota(jnp.int32, (extra_rows, LANES), 1)
    lane8 = lax.broadcasted_iota(jnp.int32, (8, LANES), 1)
    pieces = held // extra_rows
    for child in range(2):
        indices = map_ref[0, child : child + 1, :]
        hot_ref[:, child * width : (child + 1) * width] = hot(indices)
        for source in range(n):
            place = source % half
            start = source // half * span
            turned = jnp.broadcast_to(indices[:, start : start + span], (8, span))
            if place:
                turned = pltpu.roll(turned, span - place * held, 1)
            values = in_ref[source, child * held : (child + 1) * held, :]
            table = turned[:1, :LANES]
            if (place < half // 2) == (child == 0):
                extra = in_ref[source, 2 * held : 2 * held + extra_rows, :]
                values = jnp.concatenate(
                    [
                        values,
                        jnp.concatenate(
                            [jnp.where(lane // held == piece, extra, 0.0) for piece in range(pieces)], axis=0
                        ),
                    ],
                    axis=1,
                )
                far = turned[:, LANES : 2 * LANES]
                tiled = far
                for piece in range(1, pieces):
                    tiled = jnp.where(lane8 // held == piece, pltpu.roll(far, piece * held, 1), tiled)
                table = jnp.concatenate([table, tiled[:1]], axis=1)
            moved = spread(values, hot(table))
            at = child * width + source * held
            half_ref[at : at + held, :] = moved[:held]
            half_ref[2 * width + at : 2 * width + at + held, :] = moved[held:]
        other = hot(jnp.where(row // half == 0, indices[:, span:], indices[:, :span]))
        for flip in range(half):
            moved = spread(inners(flip, child), other)
            at = pl.multiple_of(child * width + (row ^ flip) * held, held)
            half_ref[pl.ds(at, held), :] += moved[:held]
            half_ref[pl.ds(2 * width + at, held), :] += moved[held:]
    for block in range(order // LANES):
        rows = pl.ds(block * LANES, LANES)
        sum_ref[rows, :] = jnp.dot(
            hot_ref[rows, :], half_ref[: 2 * width, :], preferred_element_type=f32
        ) + jnp.dot(hot_ref[rows, :], half_ref[2 * width :, :], preferred_element_type=f32)

    at = 2 * held + extra_rows
    for source in range(n):
        coup_ref[source * update_rows : (source + 1) * update_rows, :] = in_ref[
            source, at : at + update_rows, :
        ]
        aug_ref[source * pivot_rows : (source + 1) * pivot_rows, :size] = in_ref[
            source, at + update_rows : at + update_rows + pivot_rows, :
        ]
    coup_ref[...] += sum_ref[size:, :size] + sum_ref[:size, size:].T
    aug_ref[:, :size] += sum_ref[:size, :size] + sum_ref[:size, :size].T
    square = (size, size)
    aug_ref[:, size:] = jnp.where(
        lax.broadcasted_iota(jnp.int32, square, 0) == lax.broadcasted_iota(jnp.int32, square, 1), 1.0, 0.0
    )


def eliminate(aug_ref):
    size = aug_ref.shape[0]
    panel = 16
    shape = (panel, size)
    sub = lax.broadcasted_iota(jnp.int32, shape, 0)
    lane = lax.broadcasted_iota(jnp.int32, shape, 1)

    def one(block, pivots):
        base = pl.multiple_of(block * panel, panel)
        left = aug_ref[pl.ds(base, panel), :size]
        right = aug_ref[pl.ds(base, panel), size:]
        turned = pltpu.roll(left, lax.rem(size - base, size), 1)
        columns = [jnp.broadcast_to(turned[:, j : j + 1], shape) for j in range(panel)]
        scale = jnp.zeros(shape, jnp.float32)
        for j in range(panel):
            pivot = columns[j][j : j + 1, :]
            inverse = 1.0 / pivot
            multiplier = jnp.where(sub > j, columns[j] * inverse, 0.0)
            for k in range(j + 1, panel):
                columns[k] = columns[k] - multiplier * columns[k][j : j + 1, :]
            left = left - multiplier * left[j : j + 1, :]
            right = right - multiplier * right[j : j + 1, :]
            scale = jnp.where(sub == j, inverse, scale)
            pivots = jnp.where(lane[:1] == base + j, pivot, pivots)
        aug_ref[pl.ds(base, panel), :size] = left
        aug_ref[pl.ds(base, panel), size:] = right
        lower = jnp.where(lane >= base + panel, left * scale, 0.0)
        both = jnp.concatenate([left, right], axis=1)
        aug_ref[...] -= lax.dot_general(
            lower, both, (((0,), (0,)), ((), ())), precision=highest, preferred_element_type=jnp.float32
        )
        return pivots

    return lax.fori_loop(0, size // panel, one, jnp.zeros((1, size), jnp.float32))


def trailing(sum_ref, size, start):
    here = size + start
    return sum_ref[here : here + LANES, size:] + sum_ref[size:, here : here + LANES].T


LAST = (((1,), (1,)), ((), ()))


def update(out_ref, coup_ref, inverse, pivots, trailing_rows):
    size = inverse.shape[0]
    f32 = jnp.float32
    lhat = lax.dot_general(coup_ref[...], inverse, LAST, precision=highest, preferred_element_type=f32)
    out_ref[:, :size] = lhat
    coup_ref[...] = lhat / pivots
    for start in range(0, out_ref.shape[0], LANES):
        rows = pl.ds(start, LANES)
        correction = lax.dot_general(
            coup_ref[rows, :], out_ref[:, :size], LAST, precision=highest, preferred_element_type=f32
        )
        out_ref[rows, size:] = trailing_rows(start) - correction


def front_kernel(dims, row_ref, map_ref, *refs):
    n, held = dims[:2]
    outs, pivots_ref = refs[n : 2 * n], refs[2 * n]
    hot_ref, half_ref, sum_ref, aug_ref, coup_ref, in_ref, full_ref = refs[2 * n + 1 :]
    rows = in_ref.shape[1]
    for flip in range(n):
        in_ref[row_ref[0] ^ flip] = refs[flip][:rows, :]

    def inners(flip, child):
        planes = (refs[flip].shape[0] - rows) // (2 * held)
        start = rows + child * planes * held
        return jnp.concatenate(
            [refs[flip][start + plane * held : start + (plane + 1) * held, :] for plane in range(planes)], axis=1
        )

    assemble(dims, row_ref[0], map_ref, in_ref, inners, hot_ref, half_ref, sum_ref, aug_ref, coup_ref)
    size = aug_ref.shape[0]
    pivots = eliminate(aug_ref)
    pivots_ref[...] = pivots
    update(full_ref, coup_ref, aug_ref[:, size:], pivots, functools.partial(trailing, sum_ref, size))
    update_rows = outs[0].shape[0]
    for flip, out_ref in enumerate(outs):
        at = pl.multiple_of((row_ref[0] ^ flip) * update_rows, 8)
        out_ref[...] = full_ref[pl.ds(at, update_rows), :]


def factor_kernel(dims, row_ref, map_ref, in_ref, *refs):
    half = dims[0] // 2
    trail_ref, coup_ref, inverse_ref, pivots_ref, hot_ref, half_ref, sum_ref, aug_ref = refs[half:]
    inners = lambda flip, child: refs[flip][child]
    assemble(dims, row_ref[0], map_ref, in_ref, inners, hot_ref, half_ref, sum_ref, aug_ref, coup_ref)
    size = aug_ref.shape[0]
    pivots_ref[...] = eliminate(aug_ref)
    inverse_ref[...] = aug_ref[:, size:]
    for start in range(0, trail_ref.shape[0], LANES):
        trail_ref[pl.ds(start, LANES), :] = trailing(sum_ref, size, start)


def schur_kernel(row_ref, count_ref, trail_ref, coup_in_ref, inverse_ref, pivots_ref, *refs):
    out_refs = refs[:-2]
    full_ref, coup_ref = refs[-2:]
    coup_ref[...] = coup_in_ref[...]
    update(
        full_ref, coup_ref, inverse_ref[...], pivots_ref[...], lambda start: trail_ref[pl.ds(start, LANES), :]
    )
    update_rows, order = out_refs[0].shape
    size = inverse_ref.shape[0]
    shape = (8, order)
    first = lax.broadcasted_iota(jnp.int32, shape, 0)
    second = lax.broadcasted_iota(jnp.int32, shape, 1)
    for flip, out_ref in enumerate(out_refs):
        home = row_ref[0] ^ flip
        at = pl.multiple_of(home * update_rows, 8)
        out_ref[...] = full_ref[pl.ds(at, update_rows), :]
        chosen = (first == 1) & (second == size + at)
        out_ref[:8, :] = jnp.where(chosen, count_ref[0], full_ref[pl.ds(at, 8), :])


def last_kernel(size, count, stamped, row_ref, update_ref, *refs):
    back_refs, seen_ref = refs[:count], refs[count]
    lhat_ref, schur_ref, total_ref = refs[-3:]
    step = pl.program_id(0)
    update_rows, order = back_refs[0].shape
    shape = (8, order - size)
    first = lax.broadcasted_iota(jnp.int32, shape, 0)
    second = lax.broadcasted_iota(jnp.int32, shape, 1)
    at = row_ref[0] * update_rows

    @pl.when(step == 0)
    def _():
        total_ref[...] = seen_ref[...]

    for which in range(count):

        @pl.when(step == which)
        def _(which=which):
            back = back_refs[which]
            lhat_ref[0] = back[:, :size]
            schur_ref[0] = update_ref[0, :, size:] + back[:, size:]
            if not stamped:
                return
            head = back[:8, size:]
            marked = (first == 1) & (second == at)
            twin = jnp.sum(jnp.where((first == 0) & (second == at + 1), head, 0.0))
            total_ref[...] += jnp.sum(jnp.where(marked, head, 0.0))
            schur_ref[0, :8, :] = update_ref[0, :8, size:] + jnp.where(marked, twin, head)


def local_body(front_pivot, front_update, child_blocks, child_map):
    f32 = jnp.float32
    n = lax.axis_size("row")
    half = n // 2
    my_row = lax.axis_index("row")
    fronts, pivot_rows, size = front_pivot.shape
    update_rows, order = front_update.shape[1:]
    held, width = child_blocks.shape[2:]
    per = fronts // n
    span = half * held
    extra_rows = held * held // LANES
    rows = 2 * held + extra_rows + update_rows + pivot_rows
    row_number = my_row.astype(jnp.int32).reshape(1)
    dims = (n, held, extra_rows)
    group = n // 2
    vmem = pl.BlockSpec(memory_space=pltpu.VMEM)
    whole = pl.BlockSpec(memory_space=pl.ANY)
    updates = front_update.reshape(n, per, update_rows, order)
    flat = jax.ShapeDtypeStruct

    def pack(turn):
        return pl.pallas_call(
            functools.partial(pack_kernel, dims),
            grid_spec=pltpu.PrefetchScalarGridSpec(
                num_scalar_prefetch=1,
                grid=(n // group,),
                in_specs=[
                    pl.BlockSpec((group, 1, 2, held, span), lambda g, r: (g, turn, 0, 0, r[0] // half)),
                    pl.BlockSpec((group, 1, update_rows, size), lambda g, r: (g, turn, 0, 0)),
                    pl.BlockSpec((group, 1, pivot_rows, size), lambda g, r: (g, turn, 0, 0)),
                ],
                out_specs=pl.BlockSpec((group, rows, LANES), lambda g, r: (g, 0, 0)),
            ),
            out_shape=flat((n, rows, LANES), f32),
            name="pack",
        )(
            row_number,
            child_blocks.reshape(n, per, 2, held, width),
            updates,
            front_pivot.reshape(n, per, pivot_rows, size),
        )

    def parts_for(turn, flips):
        near = flips[0] < half

        def front(r, flip):
            return (r[0] ^ flip) * per + turn

        specs = [
            pl.BlockSpec((1, 2, held, span), lambda g, r, f=f: (front(r, f), 0, 0, r[0] // half)) for f in flips
        ]
        specs += [pl.BlockSpec((1, update_rows, size), lambda g, r, f=f: (front(r, f), 0, 0)) for f in flips]
        specs += [pl.BlockSpec((1, pivot_rows, size), lambda g, r, f=f: (front(r, f), 0, 0)) for f in flips]
        if near:
            specs += [
                pl.BlockSpec((1, 2, held, span), lambda g, r, f=f: (front(r, f), 0, 0, 1 - r[0] // half))
                for f in flips
            ]
        count = len(flips)
        operands = [child_blocks] * count + [front_update] * count + [front_pivot] * count
        operands += [child_blocks] * count if near else []
        return pl.pallas_call(
            functools.partial(part_kernel, dims, count),
            grid_spec=pltpu.PrefetchScalarGridSpec(
                num_scalar_prefetch=1, grid=(1,), in_specs=specs, out_specs=[vmem] * count
            ),
            out_shape=[flat((rows + (2 * held * span // LANES if near else 0), LANES), f32)] * count,
            name="parts",
        )(row_number, *operands)

    def inner(turn):
        def spec(flip):
            return pl.BlockSpec(
                (1, 2, held, span), lambda g, r: ((r[0] ^ flip) * per + turn, 0, 0, 1 - r[0] // half)
            )

        return pl.pallas_call(
            inner_kernel,
            grid_spec=pltpu.PrefetchScalarGridSpec(
                num_scalar_prefetch=1,
                grid=(1,),
                in_specs=[spec(flip) for flip in range(half)],
                out_specs=[vmem] * half,
            ),
            out_shape=[flat((2, held, span), f32)] * half,
            name="inner",
        )(row_number, *[child_blocks] * half)

    def from_arrived(kernel, arrays, turn, outs, scratch):
        return pl.pallas_call(
            functools.partial(kernel, dims + (update_rows, pivot_rows)),
            grid_spec=pltpu.PrefetchScalarGridSpec(
                num_scalar_prefetch=1,
                grid=(1,),
                in_specs=[pl.BlockSpec((1, 2, width), lambda g, r: (r[0] * per + turn, 0, 0))]
                + [vmem] * len(arrays),
                out_specs=(vmem,) * len(outs),
                scratch_shapes=[
                    pltpu.VMEM((order, 2 * width), jnp.bfloat16),
                    pltpu.VMEM((4 * width, order), jnp.bfloat16),
                    pltpu.VMEM((order, order), f32),
                    pltpu.VMEM((size, 2 * size), f32),
                ]
                + scratch,
            ),
            out_shape=tuple(flat(shape, f32) for shape in outs),
            name="front",
        )(row_number, child_map, *arrays)

    def whole_front(arrays, turn):
        outs = [(update_rows, order)] * n + [(1, size)]
        scratch = [
            pltpu.VMEM((order - size, size), f32),
            pltpu.VMEM((n, rows, LANES), f32),
            pltpu.VMEM((order - size, order), f32),
        ]
        return from_arrived(front_kernel, arrays, turn, outs, scratch)

    def factored(arrays, turn):
        outs = [(order - size, order - size), (order - size, size), (size, size), (1, size)]
        return from_arrived(factor_kernel, arrays, turn, outs, [])

    def schur_rows(count, parts):
        smem = pl.BlockSpec(memory_space=pltpu.SMEM)
        return pl.pallas_call(
            schur_kernel,
            in_specs=[smem, smem] + [vmem] * 4,
            out_specs=[vmem] * n,
            out_shape=[flat((update_rows, order), f32)] * n,
            scratch_shapes=[pltpu.VMEM((order - size, order), f32), pltpu.VMEM((order - size, size), f32)],
            name="schur",
        )(row_number, count.reshape(1), *parts)

    def last(backs, flips, turn, before, seen, stamped):
        count = len(backs)
        place = lambda g, r: ((r[0] ^ (flips[0] + g)) * per + turn, 0, 0)
        aliases = {3 + count: 0, 4 + count: 1} if before else {}
        return pl.pallas_call(
            functools.partial(last_kernel, size, count, stamped),
            grid_spec=pltpu.PrefetchScalarGridSpec(
                num_scalar_prefetch=1,
                grid=(count,),
                in_specs=[pl.BlockSpec((1, update_rows, order), place)]
                + [vmem] * (count + 1)
                + [whole] * len(before),
                out_specs=(
                    pl.BlockSpec((1, update_rows, size), place),
                    pl.BlockSpec((1, update_rows, order - size), place),
                    pl.BlockSpec((1, size), lambda g, r: (0, 0)),
                ),
            ),
            out_shape=(
                flat((fronts, update_rows, size), f32),
                flat((fronts, update_rows, order - size), f32),
                flat((1, size), f32),
            ),
            input_output_aliases=aliases,
            name="last",
        )(row_number, front_update, *backs, seen, *before)

    exchange = functools.partial(lax.all_to_all, axis_name="row", split_axis=0, concat_axis=0, tiled=True)

    def send(part, flip):
        return lax.ppermute(part, "row", [(i, i ^ flip) for i in range(n)])

    arrays = []
    for turn in range(per - 1):
        far = parts_for(turn, range(half, n))
        sent = [send(part, half + flip) for flip, part in enumerate(far[:-1])]
        far = sent + [send(far[-1], n - 1)]
        near = parts_for(turn, range(half))
        near = [near[0]] + [send(near[flip], flip) for flip in range(1, half)]
        arrays.append(near + far)
    turn = per - 1
    packed = pack(turn)
    arrived = exchange(packed)
    parts = inner(turn)
    arrays.append([arrived, parts[0]] + [send(parts[flip], flip) for flip in range(1, half)])
    total = jnp.zeros((), f32)
    backs = []

    def home(parts):
        far = [send(parts[flip], flip) for flip in range(half, n)]
        return [parts[0]] + [send(parts[flip], flip) for flip in range(1, half)] + far

    for turn in range(per - 1):
        *parts, pivots = whole_front(arrays[turn], turn)
        total = total + jnp.sum(jnp.where(pivots < 0.0, 1.0, 0.0))
        backs.append(home(parts))
    turn = per - 1
    parts = factored(arrays[turn], turn)
    total = lax.psum(total + jnp.sum(jnp.where(parts[3] < 0.0, 1.0, 0.0)), "col")
    parts = schur_rows(total, parts)
    backs.append(home(parts))
    done = ()
    seen = jnp.zeros((1, size), f32)
    singles = [range(flip, flip + 1) for flip in range(half, n)]
    cut = len(singles) // 2
    for turn in range(per):
        stamped = turn == per - 1
        groups = [range(half), range(half, n)]
        if stamped:
            groups = singles[:cut] + [range(half)] + singles[cut:]
        for flips in groups:
            lhat, schur, seen = last([backs[turn][flip] for flip in flips], flips, turn, done, seen, stamped)
            done = (lhat, schur)
    negative_share = seen[0, 0] / (fronts * lax.axis_size("col") * size)
    return (lhat, schur, negative_share)


def solution(mesh):
    in_specs = (
        P("col", "row", None),
        P("col", "row", None),
        P("col", None, "row", None),
        P("col", None, None),
    )
    out_specs = (P("col", "row", None), P("col", "row", None), P())
    return jax.shard_map(local_body, mesh=mesh, in_specs=in_specs, out_specs=out_specs, check_vma=False)
```
